512 devices in a mesh: row: 16 (over y_lo, x, core), col: 32 (over y_hi, z).
Axes of the slice: x: 4, y: 8 (y_hi: 4, y_lo: 2; y = y_hi * 2 + y_lo), z: 8, core: 2. Of those that a mesh axis runs over, the one named last changes fastest.
Arguments:
- object_field: float32 [2, 4096, 8192], P(None, 'row', 'col'), may hold values from -6 to 6
- probe: float32 [2, 128, 128], replicated, may hold values from -6 to 6
- amplitude: bfloat16 [16, 32, 16, 128, 128], P('row', 'col'), may hold values from 0 to 2
- corners: int32 [2, 16, 32, 16], P(None, 'row', 'col'), may hold values from 0 to 255, as said below
- live_count: int32 [16, 32], P('row', 'col'), may hold values from 4 to 16, as said below
Outputs:
- refined_object: float32 [2, 4096, 8192], P(None, 'row', 'col')
- new_probe: float32 [2, 128, 128], replicated
The draws below stay inside these ranges and needn't reach their ends.
Inputs may be any that keep to these rules, and one draw needn't show every extreme that they name: In the last tile row of the mesh corners[0] is at most 128, and in the last tile column corners[1] is at most 128, so every window lies inside the object. Outside the last tile row, corners[0] of slot 0 is at least 192; outside the last tile column, corners[1] of slot 0 is at least 192. Unused slots carry valid corners. Slots from live_count on are unused. Some tile uses all 16 slots in every draw.
All inputs are finite; a program needn't handle non-finite values.
Results may differ from the reference program's by a relative error of at most 0.0039.
The reference program's roundings to bfloat16 on the way count: a program that leaves them out, or rounds other values in their place, can miss the bound.
Values may be sent and summed in bfloat16 or wider, within the bound.
No kernel may reach another device: no remote copies, remote signals or barrier semaphores. Data moves between devices by JAX's collectives and lax.ppermute only.
A program may use at most 64 MiB of HBM per device.

```python
import math
import jax
import jax.numpy as jnp
from jax import lax

WIN = 128
TILE = 256
SLOTS = 16
BLOCK = 4
NR = 4096
NC = 8192
N_ROW = 16
N_COL = 32


def draw_corners(key, part):
    base_key = jax.random.fold_in(key, 11)
    first_key = jax.random.fold_in(base_key, 1)
    second_key = jax.random.fold_in(base_key, 2)
    third_key = jax.random.fold_in(base_key, 3)
    fourth_key = jax.random.fold_in(base_key, 4)
    field_shape = (N_ROW, N_COL, SLOTS)
    tile_rows = jnp.broadcast_to(jnp.arange(N_ROW, dtype=jnp.int32)[:, None, None], field_shape)
    tile_cols = jnp.broadcast_to(jnp.arange(N_COL, dtype=jnp.int32)[None, :, None], field_shape)
    slot_number = jnp.broadcast_to(jnp.arange(SLOTS, dtype=jnp.int32)[None, None, :], field_shape)
    row_limit = jnp.where(tile_rows == N_ROW - 1, TILE - WIN + 1, TILE)
    col_limit = jnp.where(tile_cols == N_COL - 1, TILE - WIN + 1, TILE)
    row_pick = jax.random.randint(first_key, field_shape, 0, row_limit)
    col_pick = jax.random.randint(second_key, field_shape, 0, col_limit)
    row_edge = TILE - WIN // 2 + jax.random.randint(third_key, field_shape, 0, WIN // 2)
    col_edge = TILE - WIN // 2 + jax.random.randint(fourth_key, field_shape, 0, WIN // 2)
    row_pick = jnp.where((slot_number == 0) & (tile_rows < N_ROW - 1), row_edge, row_pick)
    col_pick = jnp.where((slot_number == 0) & (tile_cols < N_COL - 1), col_edge, col_pick)
    return jnp.stack([row_pick, col_pick]).astype(jnp.int32)


def draw_live_count(key, part):
    base_key = jax.random.fold_in(key, 23)
    first_key = jax.random.fold_in(base_key, 1)
    second_key = jax.random.fold_in(base_key, 2)
    divisor = 1 + jax.random.randint(first_key, (N_ROW * N_COL,), 0, 4)
    counted = SLOTS // divisor
    chosen = jax.random.randint(second_key, (), 0, N_ROW * N_COL)
    counted = jnp.where(jnp.arange(N_ROW * N_COL) == chosen, SLOTS, counted)
    return counted.reshape(N_ROW, N_COL).astype(jnp.int32)


def block_levels(rng, shape, shards, least, high):
    def one(position, parts):
        draws = jax.random.uniform(jax.random.fold_in(jax.random.fold_in(rng, 6), position), (parts,), jnp.float32, least / len(shards), high / len(shards))
        return jnp.repeat(jnp.exp(draws), shape[position] // parts).reshape((-1,) + (1,) * (len(shape) - position - 1))

    loudness = one(*shards[0])
    for cut in shards[1:]:
        loudness = loudness * one(*cut)
    return loudness


def gaussian(rng, dims, scale, most, split=(), held_as=jnp.bfloat16):
    drawn = jax.random.normal(rng, dims, jnp.float32) * scale
    if len(split) > 0:
        drawn = block_levels(rng, dims, split, -0.22, 0.18) * drawn
    return jnp.clip(drawn, min=-most, max=most).astype(held_as)


def setup_inputs(seed: int = 0) -> dict:
    arg_keys = jax.random.split(jax.random.key(seed), 6)
    object_field = gaussian(arg_keys[0], (2, NR, NC), 1.0, 6.0, ((1, 16), (2, 32)), jnp.float32)
    probe = gaussian(arg_keys[1], (2, WIN, WIN), 1.0, 6.0, (), jnp.float32)
    amplitude = jnp.clip(2.0 * jax.random.uniform(arg_keys[2], (N_ROW, N_COL, SLOTS, WIN, WIN), jnp.float32) ** block_levels(arg_keys[2], (N_ROW, N_COL, SLOTS, WIN, WIN), ((0, 16), (1, 32)), -0.2, 0.2), 0.0, 2.0).astype(jnp.bfloat16)
    corners = draw_corners(jax.random.fold_in(arg_keys[5], 71), 0)
    live_count = draw_live_count(jax.random.fold_in(arg_keys[5], 71), 0)
    return {"object_field": object_field, "probe": probe, "amplitude": amplitude, "corners": corners, "live_count": live_count}


def dft_tables(window):
    indices = jnp.arange(window, dtype=jnp.int32)
    phase_index = indices[:, None] * indices[None, :] % window
    angles = phase_index.astype(jnp.float32) * (2.0 * math.pi / window)
    norming = 1.0 / math.sqrt(window)
    cosines = jnp.cos(angles) * norming
    sines = jnp.sin(angles) * norming
    forward_fourier = jnp.stack([jnp.stack([cosines, -sines]), jnp.stack([sines, cosines])])
    inverse_fourier = jnp.stack([jnp.stack([cosines, sines]), jnp.stack([-sines, cosines])])
    return (forward_fourier.astype(jnp.bfloat16), inverse_fourier.astype(jnp.bfloat16))

def times(left_value, right_value):
    real_part = left_value[..., 0, :, :] * right_value[..., 0, :, :] - left_value[..., 1, :, :] * right_value[..., 1, :, :]
    imag_part = left_value[..., 0, :, :] * right_value[..., 1, :, :] + left_value[..., 1, :, :] * right_value[..., 0, :, :]
    return jnp.stack([real_part, imag_part], -3)

def times_conj(left_value, right_value):
    real_part = left_value[..., 0, :, :] * right_value[..., 0, :, :] + left_value[..., 1, :, :] * right_value[..., 1, :, :]
    imag_part = left_value[..., 0, :, :] * right_value[..., 1, :, :] - left_value[..., 1, :, :] * right_value[..., 0, :, :]
    return jnp.stack([real_part, imag_part], -3)

def refine_object(exit_waves, measured_intensity, forward_fourier, inverse_fourier):
    highest = lax.Precision.HIGHEST
    forward_wide = forward_fourier.astype(jnp.float32)
    inverse_wide = inverse_fourier.astype(jnp.float32)
    half_done = jnp.einsum('bcrk,cdkm->bdrm', exit_waves.astype(jnp.float32), forward_wide, precision=highest).astype(jnp.bfloat16)
    spectrum = jnp.einsum('cdrs,bcsm->bdrm', forward_wide, half_done.astype(jnp.float32), precision=highest)
    modulus = jnp.sqrt(spectrum[:, 0] * spectrum[:, 0] + spectrum[:, 1] * spectrum[:, 1])
    rescale = measured_intensity.astype(jnp.float32) / jnp.maximum(modulus, 0.5)
    projected = (spectrum * rescale[:, None]).astype(jnp.bfloat16)
    half_back = jnp.einsum('bcrk,cdkm->bdrm', projected.astype(jnp.float32), inverse_wide, precision=highest).astype(jnp.bfloat16)
    returned = jnp.einsum('cdrs,bcsm->bdrm', inverse_wide, half_back.astype(jnp.float32), precision=highest)
    return returned - exit_waves.astype(jnp.float32)

def reference(object_field, probe, amplitude, corners, live_count):
    forward_fourier, inverse_fourier = dft_tables(WIN)
    tile_rows = jnp.arange(N_ROW, dtype=jnp.int32)[:, None, None] * TILE
    tile_cols = jnp.arange(N_COL, dtype=jnp.int32)[None, :, None] * TILE
    row_start = (corners[0].astype(jnp.int32) + tile_rows).reshape(-1, BLOCK)
    col_start = (corners[1].astype(jnp.int32) + tile_cols).reshape(-1, BLOCK)
    used = (jnp.arange(SLOTS, dtype=jnp.int32)[None, None, :] < live_count[:, :, None]).reshape(-1, BLOCK)
    measured_all = amplitude.reshape(-1, BLOCK, WIN, WIN)
    power = probe[0] * probe[0] + probe[1] * probe[1]
    zero_index = jnp.zeros((), jnp.int32)

    def sweep(current):

        def advance(carry, item):
            summed, lighting, gradient = carry
            starts_r, starts_c, update_marks, measured_intensity = item
            patches = jax.vmap(lambda row_at, col_at: lax.dynamic_slice(current, (zero_index, row_at, col_at), (2, WIN, WIN)))(starts_r, starts_c)
            exit_waves = times(probe[None], patches).astype(jnp.bfloat16)
            weights = update_marks.astype(jnp.float32)
            object_delta = lax.cond(jnp.any(update_marks), lambda exit_wave_portion, measurement_portion: refine_object(exit_wave_portion, measurement_portion, forward_fourier, inverse_fourier), lambda exit_wave_portion, measurement_portion: jnp.zeros(exit_wave_portion.shape, jnp.float32), exit_waves, measured_intensity)
            object_delta = object_delta * weights[:, None, None, None]
            pushed = times_conj(probe[None], object_delta)
            for member in range(BLOCK):
                anchor = (zero_index, starts_r[member], starts_c[member])
                summed = lax.dynamic_update_slice(summed, lax.dynamic_slice(summed, anchor, (2, WIN, WIN)) + pushed[member], anchor)
                flat_anchor = (starts_r[member], starts_c[member])
                lighting = lax.dynamic_update_slice(lighting, lax.dynamic_slice(lighting, flat_anchor, (WIN, WIN)) + power * weights[member], flat_anchor)
            gradient = gradient + lax.optimization_barrier(jnp.sum(times_conj(patches, object_delta), 0))
            return ((summed, lighting, gradient), None)
        start_carry = (jnp.zeros((2, NR, NC), jnp.float32), jnp.zeros((NR, NC), jnp.float32), jnp.zeros((2, WIN, WIN), jnp.float32))
        final_carry, ignored = lax.scan(advance, start_carry, (row_start, col_start, used, measured_all))
        return final_carry
    summed, lighting, first_grad = sweep(object_field)
    denominator = lighting + 4.0
    updated = object_field + summed / denominator
    summed_two, second_light, gradient = sweep(updated)
    refined_object = updated + summed_two / denominator
    spread = jnp.sqrt(jnp.mean(gradient[0] * gradient[0] + gradient[1] * gradient[1]) + 1e-06)
    new_probe = probe + gradient / spread
    return (refined_object, new_probe)
```

```python
import functools
import math

import jax
import jax.numpy as jnp
import numpy as np
from jax import lax
from jax.experimental import pallas as pl
from jax.experimental.pallas import tpu as pltpu
from jax.sharding import PartitionSpec as P

GROUP = 4
F32 = jnp.float32
BF16 = jnp.bfloat16
HALO = BF16
TERMS = BF16
GRAD = BF16


def shift(value, axis, steps):
    count = lax.axis_size(axis)
    first, last = (max(0, -steps), min(count, count - steps))
    return lax.ppermute(value, axis, [(source, source + steps) for source in range(first, last)])


def dft_tables(window):
    indices = jnp.arange(window, dtype=jnp.int32)
    phase_index = indices[:, None] * indices[None, :] % window
    angles = phase_index.astype(F32) * (2.0 * math.pi / window)
    norming = 1.0 / math.sqrt(window)
    cosines = jnp.cos(angles) * norming
    sines = jnp.sin(angles) * norming
    turned = jnp.block([[cosines, sines], [-sines, cosines]])
    straight = jnp.block([[cosines, -sines], [sines, cosines]])
    return jnp.stack([straight, turned]).astype(BF16)


def dot(left, right):
    return lax.dot_general(left, right, (((1,), (0,)), ((), ())), preferred_element_type=F32)


def accumulate(ref, lead, block, row, turn, lanes, value):
    turned = pltpu.roll(value, turn, 1)
    window = value.shape[0]
    inner = lanes >= turn
    rows = pl.ds(row, window)
    ref[lead, block, rows, :] += jnp.where(inner, turned, 0.0)
    ref[lead, block + 1, rows, :] += jnp.where(inner, 0.0, turned)


def sweep_slots(
    live_ref, corners_ref, ext_ref, probe_ref, amp_ref, tab_ref,
    dep_ref, grad_ref, power_ref, patch_ref, wave_ref, with_light,
):
    window = probe_ref.shape[1]
    live = live_ref[0, 0]
    lanes = lax.broadcasted_iota(jnp.int32, (window, window), 1)
    straight = tab_ref[0]
    turned = tab_ref[1]

    def step(index, carry):
        base = index * GROUP
        spots = []
        waves = []
        for member in range(GROUP):
            slot = base + member
            row = corners_ref[0, slot]
            col = corners_ref[1, slot]
            block = col // window
            turn = col - block * window
            spots.append((slot, row, block, turn))
            back = jnp.where(turn == 0, 0, window - turn)
            inside = lanes < window - turn
            rows = pl.ds(row, window)
            pieces = []
            for part in range(2):
                near = pltpu.roll(ext_ref[part, block, rows, :], back, 1)
                far = pltpu.roll(ext_ref[part, block + 1, rows, :], back, 1)
                pieces.append(jnp.where(inside, near, far))
            if not with_light:
                patch_ref[member, 0] = pieces[0]
                patch_ref[member, 1] = pieces[1]
            pr, pi = probe_ref[0], probe_ref[1]
            real = (pr * pieces[0] - pi * pieces[1]).astype(BF16)
            imag = (pr * pieces[1] + pi * pieces[0]).astype(BF16)
            wave = jnp.concatenate([real, imag], 1)
            wave_ref[member] = wave
            waves.append(wave)
        for pair in range(0, GROUP, 2):
            members = (pair, pair + 1)
            half = [dot(waves[m], straight).astype(BF16) for m in members]
            stacked = jnp.concatenate(
                [jnp.concatenate([h[:, :window], h[:, window:]], 0) for h in half], 1
            )
            spectrum = dot(turned, stacked)
            projected = []
            for place, m in enumerate(members):
                lo = place * window
                sr = spectrum[:window, lo : lo + window]
                si = spectrum[window:, lo : lo + window]
                amp = amp_ref[base + m].astype(F32)
                scale = amp * lax.rsqrt(jnp.maximum(sr * sr + si * si, 0.25))
                projected.append(
                    jnp.concatenate([(sr * scale).astype(BF16), (si * scale).astype(BF16)], 1)
                )
            back = [dot(p, turned).astype(BF16) for p in projected]
            stacked = jnp.concatenate(
                [jnp.concatenate([h[:, :window], h[:, window:]], 0) for h in back], 1
            )
            returned = dot(straight, stacked)
            for place, m in enumerate(members):
                slot, row, block, turn = spots[m]
                weight = jnp.where(slot < live, 1.0, 0.0).astype(F32)
                lo = place * window
                wave = wave_ref[m].astype(F32)
                cr = (returned[:window, lo : lo + window] - wave[:, :window]) * weight
                ci = (returned[window:, lo : lo + window] - wave[:, window:]) * weight
                pr, pi = probe_ref[0], probe_ref[1]
                accumulate(dep_ref, 0, block, row, turn, lanes, pr * cr + pi * ci)
                accumulate(dep_ref, 1, block, row, turn, lanes, pr * ci - pi * cr)
                if with_light:
                    accumulate(dep_ref, 2, block, row, turn, lanes, power_ref[...] * weight)
                else:
                    xr, xi = patch_ref[m, 0], patch_ref[m, 1]
                    grad_ref[0] += xr * cr + xi * ci
                    grad_ref[1] += xr * ci - xi * cr
        return carry

    lax.fori_loop(0, (live + GROUP - 1) // GROUP, step, 0)


def first_kernel(
    live_ref, corners_ref, obj_ref, right_ref, low_ref, corner_ref, probe_ref, amp_ref, tab_ref,
    ext_ref, dep_ref, to_right_ref, to_left_ref, power_ref, patch_ref, wave_ref,
):
    window = probe_ref.shape[1]
    tile = obj_ref.shape[1]
    for part in range(2):
        for block in range(2):
            cols = slice(block * window, (block + 1) * window)
            ext_ref[part, block, 0:tile, :] = obj_ref[part, :, cols]
            ext_ref[part, block, tile:, :] = low_ref[part, :, cols].astype(F32)
        ext_ref[part, 2, 0:tile, :] = right_ref[part].astype(F32)
        ext_ref[part, 2, tile:, :] = corner_ref[part].astype(F32)
    dep_ref[...] = jnp.zeros(dep_ref.shape, F32)
    power_ref[...] = probe_ref[0] * probe_ref[0] + probe_ref[1] * probe_ref[1]
    sweep_slots(
        live_ref, corners_ref, ext_ref, probe_ref, amp_ref, tab_ref,
        dep_ref, None, power_ref, patch_ref, wave_ref, True,
    )
    for part in range(3):
        to_right_ref[part] = dep_ref[part, 2].astype(TERMS)
        to_left_ref[part] = dep_ref[part, 0].astype(TERMS)


def middle_kernel(dep_ref, from_left_ref, from_right_ref, down_ref, up_ref):
    window = from_left_ref.shape[2]
    tile = from_left_ref.shape[1] - window
    for part in range(3):
        for ref, rows in ((down_ref, slice(tile, tile + window)), (up_ref, slice(0, window))):
            ref[part, 0] = (dep_ref[part, 0, rows, :] + from_left_ref[part, rows, :].astype(F32)).astype(TERMS)
            ref[part, 1] = dep_ref[part, 1, rows, :].astype(TERMS)
            ref[part, 2] = (dep_ref[part, 2, rows, :] + from_right_ref[part, rows, :].astype(F32)).astype(TERMS)


def second_kernel(
    live_ref, corners_ref, ext_ref, dep_in_ref, left_ref, right_ref, above_ref, below_ref,
    probe_ref, amp_ref, tab_ref,
    upd_ref, den_ref, dep_ref, to_right_ref, grad_ref, sum_ref, patch_ref, wave_ref,
):
    window = probe_ref.shape[1]
    total = ext_ref.shape[2]
    tile = total - window
    for block in range(3):
        for first in range(0, total, window):
            rows = slice(first, first + window)
            sums = []
            for part in (2, 0, 1):
                value = dep_in_ref[part, block, rows, :]
                if block == 0:
                    value = value + left_ref[part, rows, :].astype(F32)
                if block == 2:
                    value = value + right_ref[part, rows, :].astype(F32)
                if first == 0:
                    value = value + above_ref[part, block].astype(F32)
                if first == tile:
                    value = value + below_ref[part, block].astype(F32)
                sums.append(value)
            inverse = 1.0 / (sums[0] + 4.0)
            for part in range(2):
                upd_ref[part, block, rows, :] = ext_ref[part, block, rows, :] + sums[part + 1] * inverse
            if first < tile and block < 2:
                den_ref[block, rows, :] = inverse
    dep_ref[...] = jnp.zeros(dep_ref.shape, F32)
    grad_ref[...] = jnp.zeros(grad_ref.shape, F32)
    sweep_slots(
        live_ref, corners_ref, upd_ref, probe_ref, amp_ref, tab_ref,
        dep_ref, grad_ref, None, patch_ref, wave_ref, False,
    )
    for part in range(2):
        to_right_ref[part] = dep_ref[part, 2].astype(TERMS)


def finish_kernel(upd_ref, den_ref, dep_ref, left_ref, above_ref, out_ref):
    window = left_ref.shape[2]
    tile = out_ref.shape[1]
    for part in range(2):
        for block in range(2):
            cols = slice(block * window, (block + 1) * window)
            for first in range(0, tile, window):
                rows = slice(first, first + window)
                value = dep_ref[part, block, rows, :]
                if block == 0:
                    value = value + left_ref[part, rows, :].astype(F32)
                if first == 0:
                    value = value + above_ref[part, block].astype(F32)
                out_ref[part, rows, cols] = (
                    upd_ref[part, block, rows, :] + value * den_ref[block, rows, :]
                )


VM = pl.BlockSpec(memory_space=pltpu.VMEM)
SM = pl.BlockSpec(memory_space=pltpu.SMEM)


def call(kernel, shapes, in_specs, scratch=(), name=None, flops=10**6):
    return pl.pallas_call(
        kernel,
        out_shape=[jax.ShapeDtypeStruct(shape, kind) for shape, kind in shapes],
        in_specs=in_specs,
        out_specs=[VM] * len(shapes),
        scratch_shapes=scratch,
        name=name,
        compiler_params=pltpu.CompilerParams(vmem_limit_bytes=40 * 2**20),
        cost_estimate=pl.CostEstimate(flops=flops, transcendentals=0, bytes_accessed=10**6),
    )


def exchange(parts, axis):
    return lax.all_to_all(parts, axis, 0, 0, tiled=True)


def total_gradient(gradient):
    rows, cols = lax.axis_size("row"), lax.axis_size("col")
    lanes = gradient.shape[-1]
    parts = exchange(gradient.astype(GRAD).reshape(rows, -1, lanes), "row")
    part = jnp.sum(parts.astype(F32), 0).astype(GRAD)
    parts = exchange(jnp.broadcast_to(part[None], (cols,) + part.shape), "col")
    part = jnp.sum(parts.astype(F32), 0)
    parts = exchange(jnp.broadcast_to(part[None], (rows,) + part.shape), "row")
    return parts.reshape(gradient.shape)


def on_device(object_field, probe, amplitude, corners, live_count):
    slots = amplitude.shape[2]
    window = probe.shape[1]
    tile = object_field.shape[1]
    wide = tile + window
    across = lax.axis_size("col")
    amp = amplitude.reshape(slots, window, window)
    spots = corners.reshape(2, slots)
    live = live_count.reshape(1, 1)
    tables = dft_tables(window)

    right = shift(object_field[:, :, :window].astype(HALO), "col", -1)
    low = shift(object_field[:, :window, :].astype(HALO), "row", -1)
    diagonal = shift(
        object_field[:, :window, :window].astype(HALO), ("row", "col"), -(across + 1)
    )
    scratch = [
        pltpu.VMEM((window, window), F32),
        pltpu.VMEM((GROUP, 2, window, window), F32),
        pltpu.VMEM((GROUP, window, 2 * window), BF16),
    ]
    ext, dep, to_right, to_left = call(
        first_kernel,
        [
            ((2, 3, wide, window), F32),
            ((3, 3, wide, window), F32),
            ((3, wide, window), TERMS),
            ((3, wide, window), TERMS),
        ],
        [SM, SM] + [VM] * 7,
        scratch,
        "first_sweep",
        10**9,
    )(live, spots, object_field, right, low, diagonal, probe, amp, tables)

    from_left = shift(to_right, "col", 1)
    from_right = shift(to_left, "col", -1)
    down, up = call(
        middle_kernel,
        [((3, 3, window, window), TERMS), ((3, 3, window, window), TERMS)],
        [VM] * 3,
        name="middle",
    )(dep, from_left, from_right)
    from_above = shift(down, "row", 1)
    from_below = shift(up, "row", -1)

    updated, inverse, dep, to_right, gradient = call(
        second_kernel,
        [
            ((2, 3, wide, window), F32),
            ((2, tile, window), F32),
            ((2, 3, wide, window), F32),
            ((2, wide, window), TERMS),
            ((2, window, window), F32),
        ],
        [SM, SM] + [VM] * 9,
        scratch,
        "second_sweep",
        10**9,
    )(live, spots, ext, dep, from_left, from_right, from_above, from_below, probe, amp, tables)

    summed = total_gradient(gradient)
    from_left = shift(to_right, "col", 1)
    spill = dep[:, :2, tile:, :]
    spill = jnp.concatenate(
        [(spill[:, :1] + from_left[:, None, tile:].astype(F32)), spill[:, 1:]], 1
    ).astype(TERMS)
    from_above = shift(spill, "row", 1)
    refined = call(
        finish_kernel, [((2, tile, tile), F32)], [VM] * 5, name="finish"
    )(updated, inverse, dep, from_left, from_above)[0]
    spread = jnp.sqrt(jnp.mean(summed[0] * summed[0] + summed[1] * summed[1]) + 1e-06)
    new_probe = probe + summed / spread
    return (refined, new_probe)


def solution(mesh):
    in_specs = (
        P(None, "row", "col"),
        P(),
        P("row", "col", None, None, None),
        P(None, "row", "col", None),
        P("row", "col"),
    )
    out_specs = (P(None, "row", "col"), P())
    return jax.shard_map(
        on_device, mesh=mesh, in_specs=in_specs, out_specs=out_specs, check_vma=False
    )
```

```python
import functools
import math

import jax
import jax.numpy as jnp
import numpy as np
from jax import lax
from jax.experimental import pallas as pl
from jax.experimental.pallas import tpu as pltpu
from jax.sharding import PartitionSpec as P

GROUP = 4
F32 = jnp.float32
BF16 = jnp.bfloat16
HALO = BF16
TERMS = BF16
GRAD = BF16


def hand(value, down, right):
    rows, cols = lax.axis_size("row"), lax.axis_size("col")
    pairs = [
        (r * cols + c, (r + down) * cols + c + right)
        for r in range(max(0, -down), min(rows, rows - down))
        for c in range(max(0, -right), min(cols, cols - right))
    ]
    return lax.ppermute(value, ("row", "col"), pairs)


WAYS = ((0, 1), (0, -1), (1, 0), (-1, 0), (1, 1), (-1, -1), (1, -1), (-1, 1))
SENT = {1: (2, 3), -1: (0, 1), 0: (0, 3)}
TAKEN = {1: 0, -1: 2, 0: None}


def dft_tables(window):
    indices = jnp.arange(window, dtype=jnp.int32)
    phase_index = indices[:, None] * indices[None, :] % window
    angles = phase_index.astype(F32) * (2.0 * math.pi / window)
    norming = 1.0 / math.sqrt(window)
    cosines = jnp.cos(angles) * norming
    sines = jnp.sin(angles) * norming
    turned = jnp.block([[cosines, sines], [-sines, cosines]])
    straight = jnp.block([[cosines, -sines], [sines, cosines]])
    return jnp.stack([straight, turned]).astype(BF16)


def dot(left, right):
    return lax.dot_general(left, right, (((1,), (0,)), ((), ())), preferred_element_type=F32)


def accumulate(ref, lead, block, row, turn, lanes, value):
    turned = pltpu.roll(value, turn, 1)
    window = value.shape[0]
    inner = lanes >= turn
    rows = pl.ds(row, window)
    ref[lead, block, rows, :] += jnp.where(inner, turned, 0.0)
    ref[lead, block + 1, rows, :] += jnp.where(inner, 0.0, turned)


def sweep_slots(
    live_ref, corners_ref, ext_ref, probe_ref, amp_ref, tab_ref,
    dep_ref, grad_ref, power_ref, patch_ref, wave_ref, with_light,
):
    window = probe_ref.shape[1]
    live = live_ref[0, 0]
    lanes = lax.broadcasted_iota(jnp.int32, (window, window), 1)
    straight = tab_ref[0]
    turned = tab_ref[1]

    def step(index, carry):
        base = index * GROUP
        spots = []
        waves = []
        for member in range(GROUP):
            slot = base + member
            row = corners_ref[0, slot]
            col = corners_ref[1, slot]
            block = col // window
            turn = col - block * window
            spots.append((slot, row, block, turn))
            back = jnp.where(turn == 0, 0, window - turn)
            inside = lanes < window - turn
            rows = pl.ds(row, window)
            pieces = []
            for part in range(2):
                near = pltpu.roll(ext_ref[part, block, rows, :], back, 1)
                far = pltpu.roll(ext_ref[part, block + 1, rows, :], back, 1)
                pieces.append(jnp.where(inside, near, far))
            if not with_light:
                patch_ref[member, 0] = pieces[0]
                patch_ref[member, 1] = pieces[1]
            pr, pi = probe_ref[0], probe_ref[1]
            real = (pr * pieces[0] - pi * pieces[1]).astype(BF16)
            imag = (pr * pieces[1] + pi * pieces[0]).astype(BF16)
            wave = jnp.concatenate([real, imag], 1)
            wave_ref[member] = wave
            waves.append(wave)
        for pair in range(0, GROUP, 2):
            members = (pair, pair + 1)
            half = [dot(waves[m], straight).astype(BF16) for m in members]
            stacked = jnp.concatenate(
                [jnp.concatenate([h[:, :window], h[:, window:]], 0) for h in half], 1
            )
            spectrum = dot(turned, stacked)
            projected = []
            for place, m in enumerate(members):
                lo = place * window
                sr = spectrum[:window, lo : lo + window]
                si = spectrum[window:, lo : lo + window]
                amp = amp_ref[base + m].astype(F32)
                scale = amp * lax.rsqrt(jnp.maximum(sr * sr + si * si, 0.25))
                projected.append(
                    jnp.concatenate([(sr * scale).astype(BF16), (si * scale).astype(BF16)], 1)
                )
            back = [dot(p, turned).astype(BF16) for p in projected]
            stacked = jnp.concatenate(
                [jnp.concatenate([h[:, :window], h[:, window:]], 0) for h in back], 1
            )
            returned = dot(straight, stacked)
            for place, m in enumerate(members):
                slot, row, block, turn = spots[m]
                weight = jnp.where(slot < live, 1.0, 0.0).astype(F32)
                lo = place * window
                wave = wave_ref[m].astype(F32)
                cr = (returned[:window, lo : lo + window] - wave[:, :window]) * weight
                ci = (returned[window:, lo : lo + window] - wave[:, window:]) * weight
                pr, pi = probe_ref[0], probe_ref[1]
                accumulate(dep_ref, 0, block, row, turn, lanes, pr * cr + pi * ci)
                accumulate(dep_ref, 1, block, row, turn, lanes, pr * ci - pi * cr)
                if with_light:
                    accumulate(dep_ref, 2, block, row, turn, lanes, power_ref[...] * weight)
                else:
                    xr, xi = patch_ref[m, 0], patch_ref[m, 1]
                    grad_ref[0] += xr * cr + xi * ci
                    grad_ref[1] += xr * ci - xi * cr
        return carry

    lax.fori_loop(0, (live + GROUP - 1) // GROUP, step, 0)


def first_kernel(
    live_ref, corners_ref, obj_ref, right_ref, low_ref, corner_ref, probe_ref, amp_ref, tab_ref,
    ext_ref, dep_ref, *rest,
):
    leaving, (power_ref, patch_ref, wave_ref) = rest[: len(WAYS)], rest[len(WAYS) :]
    window = probe_ref.shape[1]
    tile = obj_ref.shape[1]
    for part in range(2):
        for block in range(2):
            cols = slice(block * window, (block + 1) * window)
            ext_ref[part, block, 0:tile, :] = obj_ref[part, :, cols]
            ext_ref[part, block, tile:, :] = low_ref[part, :, cols].astype(F32)
        ext_ref[part, 2, 0:tile, :] = right_ref[part].astype(F32)
        ext_ref[part, 2, tile:, :] = corner_ref[part].astype(F32)
    dep_ref[...] = jnp.zeros(dep_ref.shape, F32)
    power_ref[...] = probe_ref[0] * probe_ref[0] + probe_ref[1] * probe_ref[1]
    sweep_slots(
        live_ref, corners_ref, ext_ref, probe_ref, amp_ref, tab_ref,
        dep_ref, None, power_ref, patch_ref, wave_ref, True,
    )
    for (down, right), ref in zip(WAYS, leaving):
        first, last = SENT[down]
        low, high = SENT[right]
        ref[...] = dep_ref[:, low:high, first * window : last * window, :].astype(TERMS)


def second_kernel(
    live_ref, corners_ref, ext_ref, dep_in_ref, probe_ref, amp_ref, tab_ref, *rest,
):
    arrived = rest[: len(WAYS)]
    upd_ref, den_ref, dep_ref, right_ref, low_ref, corner_ref, grad_ref = rest[len(WAYS) : -2]
    patch_ref, wave_ref = rest[-2:]
    window = probe_ref.shape[1]
    total = ext_ref.shape[2]
    tile = total - window
    for block in range(3):
        for first in range(0, total, window):
            rows = slice(first, first + window)
            sums = []
            for part in (2, 0, 1):
                value = dep_in_ref[part, block, rows, :]
                for (down, right), ref in zip(WAYS, arrived):
                    if TAKEN[right] not in (None, block) or TAKEN[down] not in (None, first // window):
                        continue
                    place = block if right == 0 else 0
                    start = first if down == 0 else 0
                    value = value + ref[part, place, start : start + window, :].astype(F32)
                sums.append(value)
            inverse = 1.0 / (sums[0] + 4.0)
            for part in range(2):
                upd_ref[part, block, rows, :] = ext_ref[part, block, rows, :] + sums[part + 1] * inverse
            if first < tile and block < 2:
                den_ref[block, rows, :] = inverse
    dep_ref[...] = jnp.zeros(dep_ref.shape, F32)
    grad_ref[...] = jnp.zeros(grad_ref.shape, F32)
    sweep_slots(
        live_ref, corners_ref, upd_ref, probe_ref, amp_ref, tab_ref,
        dep_ref, grad_ref, None, patch_ref, wave_ref, False,
    )
    right_ref[...] = dep_ref[:, 2, :tile, :].astype(TERMS)
    low_ref[...] = dep_ref[:, :2, tile:, :].astype(TERMS)
    corner_ref[...] = dep_ref[:, 2, tile:, :].astype(TERMS)


def finish_kernel(upd_ref, den_ref, dep_ref, left_ref, above_ref, corner_ref, out_ref):
    window = left_ref.shape[2]
    tile = out_ref.shape[1]
    for part in range(2):
        for block in range(2):
            cols = slice(block * window, (block + 1) * window)
            for first in range(0, tile, window):
                rows = slice(first, first + window)
                value = dep_ref[part, block, rows, :]
                if block == 0:
                    value = value + left_ref[part, rows, :].astype(F32)
                if first == 0:
                    value = value + above_ref[part, block].astype(F32)
                if block == 0 and first == 0:
                    value = value + corner_ref[part].astype(F32)
                out_ref[part, rows, cols] = (
                    upd_ref[part, block, rows, :] + value * den_ref[block, rows, :]
                )


VM = pl.BlockSpec(memory_space=pltpu.VMEM)
SM = pl.BlockSpec(memory_space=pltpu.SMEM)


def call(kernel, shapes, in_specs, scratch=(), name=None, flops=10**6):
    return pl.pallas_call(
        kernel,
        out_shape=[jax.ShapeDtypeStruct(shape, kind) for shape, kind in shapes],
        in_specs=in_specs,
        out_specs=[VM] * len(shapes),
        scratch_shapes=scratch,
        name=name,
        compiler_params=pltpu.CompilerParams(vmem_limit_bytes=40 * 2**20),
        cost_estimate=pl.CostEstimate(flops=flops, transcendentals=0, bytes_accessed=10**6),
    )


def exchange(parts, axis):
    return lax.all_to_all(parts, axis, 0, 0, tiled=True)


def on_device(object_field, probe, amplitude, corners, live_count):
    slots = amplitude.shape[2]
    window = probe.shape[1]
    tile = object_field.shape[1]
    wide = tile + window
    rows, cols = lax.axis_size("row"), lax.axis_size("col")
    amp = amplitude.reshape(slots, window, window)
    spots = corners.reshape(2, slots)
    live = live_count.reshape(1, 1)
    tables = dft_tables(window)

    right = hand(object_field[:, :, :window].astype(HALO), 0, -1)
    low = hand(object_field[:, :window, :].astype(HALO), -1, 0)
    diagonal = hand(object_field[:, :window, :window].astype(HALO), -1, -1)
    scratch = [
        pltpu.VMEM((GROUP, 2, window, window), F32),
        pltpu.VMEM((GROUP, window, 2 * window), BF16),
    ]
    leaving = [
        ((3, SENT[r][1] - SENT[r][0], (SENT[d][1] - SENT[d][0]) * window, window), TERMS)
        for d, r in WAYS
    ]
    ext, dep, *terms = call(
        first_kernel,
        [((2, 3, wide, window), F32), ((3, 3, wide, window), F32)] + leaving,
        [SM, SM] + [VM] * 7,
        [pltpu.VMEM((window, window), F32)] + scratch,
        "first_sweep",
        10**9,
    )(live, spots, object_field, right, low, diagonal, probe, amp, tables)
    terms = [hand(term, *way) for term, way in zip(terms, WAYS)]
    updated, inverse, dep, to_right, to_low, to_corner, gradient = call(
        second_kernel,
        [
            ((2, 3, wide, window), F32),
            ((2, tile, window), F32),
            ((2, 3, wide, window), F32),
            ((2, tile, window), TERMS),
            ((2, 2, window, window), TERMS),
            ((2, window, window), TERMS),
            ((2, window, window), F32),
        ],
        [SM, SM] + [VM] * (5 + len(WAYS)),
        scratch,
        "second_sweep",
        10**9,
    )(live, spots, ext, dep, probe, amp, tables, *terms)

    parts = exchange(gradient.astype(GRAD).reshape(rows, -1, window), "row")
    part = jnp.sum(parts.astype(F32), 0).astype(GRAD)
    part, to_right, to_low, to_corner = lax.optimization_barrier(
        (part, to_right, to_low, to_corner)
    )
    parts = exchange(jnp.broadcast_to(part[None], (cols,) + part.shape), "col")
    from_left = hand(to_right, 0, 1)
    from_above = hand(to_low, 1, 0)
    from_corner = hand(to_corner, 1, 1)
    refined = call(finish_kernel, [((2, tile, tile), F32)], [VM] * 6, name="finish")(
        updated, inverse, dep, from_left, from_above, from_corner
    )[0]
    parts, refined = lax.optimization_barrier((parts, refined))
    part = jnp.sum(parts.astype(F32), 0)
    parts = exchange(jnp.broadcast_to(part[None], (rows,) + part.shape), "row")
    summed = parts.reshape(gradient.shape)
    spread = jnp.sqrt(jnp.mean(summed[0] * summed[0] + summed[1] * summed[1]) + 1e-06)
    new_probe = probe + summed / spread
    return (refined, new_probe)


def solution(mesh):
    in_specs = (
        P(None, "row", "col"),
        P(),
        P("row", "col", None, None, None),
        P(None, "row", "col", None),
        P("row", "col"),
    )
    out_specs = (P(None, "row", "col"), P())
    return jax.shard_map(
        on_device, mesh=mesh, in_specs=in_specs, out_specs=out_specs, check_vma=False
    )
```

```python
import functools
import math

import jax
import jax.numpy as jnp
import numpy as np
from jax import lax
from jax.experimental import pallas as pl
from jax.experimental.pallas import tpu as pltpu
from jax.sharding import PartitionSpec as P

GROUP = 4
F32 = jnp.float32
BF16 = jnp.bfloat16
HALO = BF16
TERMS = BF16
GRAD = BF16


def shift(value, axis, steps):
    count = lax.axis_size(axis)
    first, last = (max(0, -steps), min(count, count - steps))
    return lax.ppermute(value, axis, [(source, source + steps) for source in range(first, last)])


def dft_tables(window):
    indices = jnp.arange(window, dtype=jnp.int32)
    phase_index = indices[:, None] * indices[None, :] % window
    angles = phase_index.astype(F32) * (2.0 * math.pi / window)
    norming = 1.0 / math.sqrt(window)
    cosines = jnp.cos(angles) * norming
    sines = jnp.sin(angles) * norming
    turned = jnp.block([[cosines, sines], [-sines, cosines]])
    straight = jnp.block([[cosines, -sines], [sines, cosines]])
    return jnp.stack([straight, turned]).astype(BF16)


def dot(left, right):
    return lax.dot_general(left, right, (((1,), (0,)), ((), ())), preferred_element_type=F32)


def accumulate(ref, lead, block, row, turn, lanes, value):
    turned = pltpu.roll(value, turn, 1)
    window = value.shape[0]
    inner = lanes >= turn
    rows = pl.ds(row, window)
    ref[lead, block, rows, :] += jnp.where(inner, turned, 0.0)
    ref[lead, block + 1, rows, :] += jnp.where(inner, 0.0, turned)


def sweep_slots(
    live_ref, corners_ref, ext_ref, probe_ref, amp_ref, tab_ref,
    dep_ref, grad_ref, power_ref, patch_ref, wave_ref, with_light,
):
    window = probe_ref.shape[1]
    live = live_ref[0, 0]
    lanes = lax.broadcasted_iota(jnp.int32, (window, window), 1)
    straight = tab_ref[0]
    turned = tab_ref[1]

    def step(index, carry):
        base = index * GROUP
        spots = []
        waves = []
        for member in range(GROUP):
            slot = base + member
            row = corners_ref[0, slot]
            col = corners_ref[1, slot]
            block = col // window
            turn = col - block * window
            spots.append((slot, row, block, turn))
            back = jnp.where(turn == 0, 0, window - turn)
            inside = lanes < window - turn
            rows = pl.ds(row, window)
            pieces = []
            for part in range(2):
                near = pltpu.roll(ext_ref[part, block, rows, :], back, 1)
                far = pltpu.roll(ext_ref[part, block + 1, rows, :], back, 1)
                pieces.append(jnp.where(inside, near, far))
            if not with_light:
                patch_ref[member, 0] = pieces[0]
                patch_ref[member, 1] = pieces[1]
            pr, pi = probe_ref[0], probe_ref[1]
            real = (pr * pieces[0] - pi * pieces[1]).astype(BF16)
            imag = (pr * pieces[1] + pi * pieces[0]).astype(BF16)
            wave = jnp.concatenate([real, imag], 1)
            wave_ref[member] = wave
            waves.append(wave)
        for pair in range(0, GROUP, 2):
            members = (pair, pair + 1)
            half = [dot(waves[m], straight).astype(BF16) for m in members]
            stacked = jnp.concatenate(
                [jnp.concatenate([h[:, :window], h[:, window:]], 0) for h in half], 1
            )
            spectrum = dot(turned, stacked)
            projected = []
            for place, m in enumerate(members):
                lo = place * window
                sr = spectrum[:window, lo : lo + window]
                si = spectrum[window:, lo : lo + window]
                amp = amp_ref[base + m].astype(F32)
                scale = amp * lax.rsqrt(jnp.maximum(sr * sr + si * si, 0.25))
                projected.append(
                    jnp.concatenate([(sr * scale).astype(BF16), (si * scale).astype(BF16)], 1)
                )
            back = [dot(p, turned).astype(BF16) for p in projected]
            stacked = jnp.concatenate(
                [jnp.concatenate([h[:, :window], h[:, window:]], 0) for h in back], 1
            )
            returned = dot(straight, stacked)
            for place, m in enumerate(members):
                slot, row, block, turn = spots[m]
                weight = jnp.where(slot < live, 1.0, 0.0).astype(F32)
                lo = place * window
                wave = wave_ref[m].astype(F32)
                cr = (returned[:window, lo : lo + window] - wave[:, :window]) * weight
                ci = (returned[window:, lo : lo + window] - wave[:, window:]) * weight
                pr, pi = probe_ref[0], probe_ref[1]
                accumulate(dep_ref, 0, block, row, turn, lanes, pr * cr + pi * ci)
                accumulate(dep_ref, 1, block, row, turn, lanes, pr * ci - pi * cr)
                if with_light:
                    accumulate(dep_ref, 2, block, row, turn, lanes, power_ref[...] * weight)
                else:
                    xr, xi = patch_ref[m, 0], patch_ref[m, 1]
                    grad_ref[0] += xr * cr + xi * ci
                    grad_ref[1] += xr * ci - xi * cr
        return carry

    lax.fori_loop(0, (live + GROUP - 1) // GROUP, step, 0)


def first_kernel(
    live_ref, corners_ref, obj_ref, right_ref, low_ref, corner_ref, probe_ref, amp_ref, tab_ref,
    ext_ref, dep_ref, to_right_ref, to_left_ref, power_ref, patch_ref, wave_ref,
):
    window = probe_ref.shape[1]
    tile = obj_ref.shape[1]
    for part in range(2):
        for block in range(2):
            cols = slice(block * window, (block + 1) * window)
            ext_ref[part, block, 0:tile, :] = obj_ref[part, :, cols]
            ext_ref[part, block, tile:, :] = low_ref[part, :, cols].astype(F32)
        ext_ref[part, 2, 0:tile, :] = right_ref[part].astype(F32)
        ext_ref[part, 2, tile:, :] = corner_ref[part].astype(F32)
    dep_ref[...] = jnp.zeros(dep_ref.shape, F32)
    power_ref[...] = probe_ref[0] * probe_ref[0] + probe_ref[1] * probe_ref[1]
    sweep_slots(
        live_ref, corners_ref, ext_ref, probe_ref, amp_ref, tab_ref,
        dep_ref, None, power_ref, patch_ref, wave_ref, True,
    )
    for part in range(3):
        to_right_ref[part] = dep_ref[part, 2].astype(TERMS)
        to_left_ref[part] = dep_ref[part, 0].astype(TERMS)


def middle_kernel(dep_ref, from_left_ref, from_right_ref, down_ref, up_ref):
    window = from_left_ref.shape[2]
    tile = from_left_ref.shape[1] - window
    for part in range(3):
        for ref, rows in ((down_ref, slice(tile, tile + window)), (up_ref, slice(0, window))):
            ref[part, 0] = (dep_ref[part, 0, rows, :] + from_left_ref[part, rows, :].astype(F32)).astype(TERMS)
            ref[part, 1] = dep_ref[part, 1, rows, :].astype(TERMS)
            ref[part, 2] = (dep_ref[part, 2, rows, :] + from_right_ref[part, rows, :].astype(F32)).astype(TERMS)


def second_kernel(
    live_ref, corners_ref, ext_ref, dep_in_ref, left_ref, right_ref, above_ref, below_ref,
    probe_ref, amp_ref, tab_ref,
    upd_ref, den_ref, dep_ref, to_right_ref, grad_ref, sum_ref, patch_ref, wave_ref,
):
    window = probe_ref.shape[1]
    total = ext_ref.shape[2]
    tile = total - window
    for block in range(3):
        for first in range(0, total, window):
            rows = slice(first, first + window)
            sums = []
            for part in (2, 0, 1):
                value = dep_in_ref[part, block, rows, :]
                if block == 0:
                    value = value + left_ref[part, rows, :].astype(F32)
                if block == 2:
                    value = value + right_ref[part, rows, :].astype(F32)
                if first == 0:
                    value = value + above_ref[part, block].astype(F32)
                if first == tile:
                    value = value + below_ref[part, block].astype(F32)
                sums.append(value)
            inverse = 1.0 / (sums[0] + 4.0)
            for part in range(2):
                upd_ref[part, block, rows, :] = ext_ref[part, block, rows, :] + sums[part + 1] * inverse
            if first < tile and block < 2:
                den_ref[block, rows, :] = inverse
    dep_ref[...] = jnp.zeros(dep_ref.shape, F32)
    grad_ref[...] = jnp.zeros(grad_ref.shape, F32)
    sweep_slots(
        live_ref, corners_ref, upd_ref, probe_ref, amp_ref, tab_ref,
        dep_ref, grad_ref, None, patch_ref, wave_ref, False,
    )
    for part in range(2):
        to_right_ref[part] = dep_ref[part, 2].astype(TERMS)


def finish_kernel(upd_ref, den_ref, dep_ref, left_ref, above_ref, out_ref):
    window = left_ref.shape[2]
    tile = out_ref.shape[1]
    for part in range(2):
        for block in range(2):
            cols = slice(block * window, (block + 1) * window)
            for first in range(0, tile, window):
                rows = slice(first, first + window)
                value = dep_ref[part, block, rows, :]
                if block == 0:
                    value = value + left_ref[part, rows, :].astype(F32)
                if first == 0:
                    value = value + above_ref[part, block].astype(F32)
                out_ref[part, rows, cols] = (
                    upd_ref[part, block, rows, :] + value * den_ref[block, rows, :]
                )


VM = pl.BlockSpec(memory_space=pltpu.VMEM)
SM = pl.BlockSpec(memory_space=pltpu.SMEM)


def call(kernel, shapes, in_specs, scratch=(), name=None, flops=10**6):
    return pl.pallas_call(
        kernel,
        out_shape=[jax.ShapeDtypeStruct(shape, kind) for shape, kind in shapes],
        in_specs=in_specs,
        out_specs=[VM] * len(shapes),
        scratch_shapes=scratch,
        name=name,
        compiler_params=pltpu.CompilerParams(vmem_limit_bytes=40 * 2**20),
        cost_estimate=pl.CostEstimate(flops=flops, transcendentals=0, bytes_accessed=10**6),
    )


def exchange(parts, axis, groups=None):
    return lax.all_to_all(parts, axis, 0, 0, axis_index_groups=groups, tiled=True)


def summed_over(part, axis, groups):
    count = len(groups[0])
    parts = exchange(jnp.broadcast_to(part[None], (count,) + part.shape), axis, groups)
    return jnp.sum(parts, 0)


def near_groups(size):
    run = next(r for r in (8, 4, 2, 1) if size % r == 0)
    runs = [list(range(first, first + run)) for first in range(0, size, run)]
    return runs, [list(members) for members in zip(*runs)]


def on_device(object_field, probe, amplitude, corners, live_count):
    slots = amplitude.shape[2]
    window = probe.shape[1]
    tile = object_field.shape[1]
    wide = tile + window
    width = lax.axis_size("col")
    amp = amplitude.reshape(slots, window, window)
    spots = corners.reshape(2, slots)
    live = live_count.reshape(1, 1)
    tables = dft_tables(window)

    right = shift(object_field[:, :, :window].astype(HALO), "col", -1)
    low = shift(object_field[:, :window, :].astype(HALO), "row", -1)
    diagonal = shift(
        object_field[:, :window, :window].astype(HALO), ("row", "col"), -(width + 1)
    )
    scratch = [
        pltpu.VMEM((window, window), F32),
        pltpu.VMEM((GROUP, 2, window, window), F32),
        pltpu.VMEM((GROUP, window, 2 * window), BF16),
    ]
    ext, dep, to_right, to_left = call(
        first_kernel,
        [
            ((2, 3, wide, window), F32),
            ((3, 3, wide, window), F32),
            ((3, wide, window), TERMS),
            ((3, wide, window), TERMS),
        ],
        [SM, SM] + [VM] * 7,
        scratch,
        "first_sweep",
        10**9,
    )(live, spots, object_field, right, low, diagonal, probe, amp, tables)

    from_left = shift(to_right, "col", 1)
    from_right = shift(to_left, "col", -1)
    down, up = call(
        middle_kernel,
        [((3, 3, window, window), TERMS), ((3, 3, window, window), TERMS)],
        [VM] * 3,
        name="middle",
    )(dep, from_left, from_right)
    from_above = shift(down, "row", 1)
    from_below = shift(up, "row", -1)

    updated, inverse, dep, to_right, gradient = call(
        second_kernel,
        [
            ((2, 3, wide, window), F32),
            ((2, tile, window), F32),
            ((2, 3, wide, window), F32),
            ((2, wide, window), TERMS),
            ((2, window, window), F32),
        ],
        [SM, SM] + [VM] * 9,
        scratch,
        "second_sweep",
        10**9,
    )(live, spots, ext, dep, from_left, from_right, from_above, from_below, probe, amp, tables)

    from_left = shift(to_right, "col", 1)
    rows, cols = lax.axis_size("row"), lax.axis_size("col")
    runs, across = near_groups(cols)
    parts = exchange(gradient.astype(GRAD).reshape(rows, -1, window), "row")
    part = jnp.sum(parts.astype(F32), 0)
    part, from_left, dep = lax.optimization_barrier((part, from_left, dep))
    spill = dep[:, :2, tile:, :]
    spill = jnp.concatenate(
        [(spill[:, :1] + from_left[:, None, tile:].astype(F32)), spill[:, 1:]], 1
    ).astype(TERMS)
    part = summed_over(part, "col", across)
    from_above = shift(spill, "row", 1)
    part = summed_over(part, "col", runs)
    refined = call(
        finish_kernel, [((2, tile, tile), F32)], [VM] * 5, name="finish"
    )(updated, inverse, dep, from_left, from_above)[0]
    part, refined = lax.optimization_barrier((part, refined))
    parts = exchange(jnp.broadcast_to(part[None], (rows,) + part.shape), "row")
    summed = parts.reshape(gradient.shape)
    spread = jnp.sqrt(jnp.mean(summed[0] * summed[0] + summed[1] * summed[1]) + 1e-06)
    new_probe = probe + summed / spread
    return (refined, new_probe)


def solution(mesh):
    in_specs = (
        P(None, "row", "col"),
        P(),
        P("row", "col", None, None, None),
        P(None, "row", "col", None),
        P("row", "col"),
    )
    out_specs = (P(None, "row", "col"), P())
    return jax.shard_map(
        on_device, mesh=mesh, in_specs=in_specs, out_specs=out_specs, check_vma=False
    )
```

```python
import functools
import math

import jax
import jax.numpy as jnp
import numpy as np
from jax import lax
from jax.experimental import pallas as pl
from jax.experimental.pallas import tpu as pltpu
from jax.sharding import PartitionSpec as P

GROUP = 4
F32 = jnp.float32
BF16 = jnp.bfloat16
HALO = BF16
TERMS = BF16
GRAD = BF16


def shift(value, axis, steps):
    count = lax.axis_size(axis)
    first, last = (max(0, -steps), min(count, count - steps))
    return lax.ppermute(value, axis, [(source, source + steps) for source in range(first, last)])


def dft_tables(window):
    indices = jnp.arange(window, dtype=jnp.int32)
    phase_index = indices[:, None] * indices[None, :] % window
    angles = phase_index.astype(F32) * (2.0 * math.pi / window)
    norming = 1.0 / math.sqrt(window)
    cosines = jnp.cos(angles) * norming
    sines = jnp.sin(angles) * norming
    turned = jnp.block([[cosines, sines], [-sines, cosines]])
    straight = jnp.block([[cosines, -sines], [sines, cosines]])
    return jnp.stack([straight, turned]).astype(BF16)


def dot(left, right):
    return lax.dot_general(left, right, (((1,), (0,)), ((), ())), preferred_element_type=F32)


def accumulate(ref, lead, block, row, turn, lanes, value):
    turned = pltpu.roll(value, turn, 1)
    window = value.shape[0]
    inner = lanes >= turn
    rows = pl.ds(row, window)
    ref[lead, block, rows, :] += jnp.where(inner, turned, 0.0)
    ref[lead, block + 1, rows, :] += jnp.where(inner, 0.0, turned)


def sweep_slots(
    live_ref, corners_ref, ext_ref, probe_ref, amp_ref, tab_ref,
    dep_ref, grad_ref, power_ref, patch_ref, wave_ref, with_light,
):
    window = probe_ref.shape[1]
    live = live_ref[0, 0]
    lanes = lax.broadcasted_iota(jnp.int32, (window, window), 1)
    straight = tab_ref[0]
    turned = tab_ref[1]

    def step(index, carry):
        base = index * GROUP
        spots = []
        waves = []
        for member in range(GROUP):
            slot = base + member
            row = corners_ref[0, slot]
            col = corners_ref[1, slot]
            block = col // window
            turn = col - block * window
            spots.append((slot, row, block, turn))
            back = jnp.where(turn == 0, 0, window - turn)
            inside = lanes < window - turn
            rows = pl.ds(row, window)
            pieces = []
            for part in range(2):
                near = pltpu.roll(ext_ref[part, block, rows, :], back, 1)
                far = pltpu.roll(ext_ref[part, block + 1, rows, :], back, 1)
                pieces.append(jnp.where(inside, near, far))
            if not with_light:
                patch_ref[member, 0] = pieces[0]
                patch_ref[member, 1] = pieces[1]
            pr, pi = probe_ref[0], probe_ref[1]
            real = (pr * pieces[0] - pi * pieces[1]).astype(BF16)
            imag = (pr * pieces[1] + pi * pieces[0]).astype(BF16)
            wave = jnp.concatenate([real, imag], 1)
            wave_ref[member] = wave
            waves.append(wave)
        for pair in range(0, GROUP, 2):
            members = (pair, pair + 1)
            half = [dot(waves[m], straight).astype(BF16) for m in members]
            stacked = jnp.concatenate(
                [jnp.concatenate([h[:, :window], h[:, window:]], 0) for h in half], 1
            )
            spectrum = dot(turned, stacked)
            projected = []
            for place, m in enumerate(members):
                lo = place * window
                sr = spectrum[:window, lo : lo + window]
                si = spectrum[window:, lo : lo + window]
                amp = amp_ref[base + m].astype(F32)
                scale = amp * lax.rsqrt(jnp.maximum(sr * sr + si * si, 0.25))
                projected.append(
                    jnp.concatenate([(sr * scale).astype(BF16), (si * scale).astype(BF16)], 1)
                )
            back = [dot(p, turned).astype(BF16) for p in projected]
            stacked = jnp.concatenate(
                [jnp.concatenate([h[:, :window], h[:, window:]], 0) for h in back], 1
            )
            returned = dot(straight, stacked)
            for place, m in enumerate(members):
                slot, row, block, turn = spots[m]
                weight = jnp.where(slot < live, 1.0, 0.0).astype(F32)
                lo = place * window
                wave = wave_ref[m].astype(F32)
                cr = (returned[:window, lo : lo + window] - wave[:, :window]) * weight
                ci = (returned[window:, lo : lo + window] - wave[:, window:]) * weight
                pr, pi = probe_ref[0], probe_ref[1]
                accumulate(dep_ref, 0, block, row, turn, lanes, pr * cr + pi * ci)
                accumulate(dep_ref, 1, block, row, turn, lanes, pr * ci - pi * cr)
                if with_light:
                    accumulate(dep_ref, 2, block, row, turn, lanes, power_ref[...] * weight)
                else:
                    xr, xi = patch_ref[m, 0], patch_ref[m, 1]
                    grad_ref[0] += xr * cr + xi * ci
                    grad_ref[1] += xr * ci - xi * cr
        return carry

    lax.fori_loop(0, (live + GROUP - 1) // GROUP, step, 0)


def first_kernel(
    live_ref, corners_ref, obj_ref, right_ref, low_ref, corner_ref, probe_ref, amp_ref, tab_ref,
    ext_ref, dep_ref, to_right_ref, to_left_ref, power_ref, patch_ref, wave_ref,
):
    window = probe_ref.shape[1]
    tile = obj_ref.shape[1]
    for part in range(2):
        for block in range(2):
            cols = slice(block * window, (block + 1) * window)
            ext_ref[part, block, 0:tile, :] = obj_ref[part, :, cols]
            ext_ref[part, block, tile:, :] = low_ref[part, :, cols].astype(F32)
        ext_ref[part, 2, 0:tile, :] = right_ref[part].astype(F32)
        ext_ref[part, 2, tile:, :] = corner_ref[part].astype(F32)
    dep_ref[...] = jnp.zeros(dep_ref.shape, F32)
    power_ref[...] = probe_ref[0] * probe_ref[0] + probe_ref[1] * probe_ref[1]
    sweep_slots(
        live_ref, corners_ref, ext_ref, probe_ref, amp_ref, tab_ref,
        dep_ref, None, power_ref, patch_ref, wave_ref, True,
    )
    for part in range(3):
        to_right_ref[part] = dep_ref[part, 2].astype(TERMS)
        to_left_ref[part] = dep_ref[part, 0].astype(TERMS)


def middle_kernel(dep_ref, from_left_ref, from_right_ref, down_ref, up_ref):
    window = from_left_ref.shape[2]
    tile = from_left_ref.shape[1] - window
    for part in range(3):
        for ref, rows in ((down_ref, slice(tile, tile + window)), (up_ref, slice(0, window))):
            ref[part, 0] = (dep_ref[part, 0, rows, :] + from_left_ref[part, rows, :].astype(F32)).astype(TERMS)
            ref[part, 1] = dep_ref[part, 1, rows, :].astype(TERMS)
            ref[part, 2] = (dep_ref[part, 2, rows, :] + from_right_ref[part, rows, :].astype(F32)).astype(TERMS)


def second_kernel(
    live_ref, corners_ref, ext_ref, dep_in_ref, left_ref, right_ref, above_ref, below_ref,
    probe_ref, amp_ref, tab_ref,
    upd_ref, den_ref, dep_ref, to_right_ref, grad_ref, sum_ref, patch_ref, wave_ref,
):
    window = probe_ref.shape[1]
    total = ext_ref.shape[2]
    tile = total - window
    for block in range(3):
        for first in range(0, total, window):
            rows = slice(first, first + window)
            sums = []
            for part in (2, 0, 1):
                value = dep_in_ref[part, block, rows, :]
                if block == 0:
                    value = value + left_ref[part, rows, :].astype(F32)
                if block == 2:
                    value = value + right_ref[part, rows, :].astype(F32)
                if first == 0:
                    value = value + above_ref[part, block].astype(F32)
                if first == tile:
                    value = value + below_ref[part, block].astype(F32)
                sums.append(value)
            inverse = 1.0 / (sums[0] + 4.0)
            for part in range(2):
                upd_ref[part, block, rows, :] = ext_ref[part, block, rows, :] + sums[part + 1] * inverse
            if first < tile and block < 2:
                den_ref[block, rows, :] = inverse
    dep_ref[...] = jnp.zeros(dep_ref.shape, F32)
    grad_ref[...] = jnp.zeros(grad_ref.shape, F32)
    sweep_slots(
        live_ref, corners_ref, upd_ref, probe_ref, amp_ref, tab_ref,
        dep_ref, grad_ref, None, patch_ref, wave_ref, False,
    )
    for part in range(2):
        to_right_ref[part] = dep_ref[part, 2].astype(TERMS)


def finish_kernel(upd_ref, den_ref, dep_ref, left_ref, above_ref, out_ref):
    window = left_ref.shape[2]
    tile = out_ref.shape[1]
    for part in range(2):
        for block in range(2):
            cols = slice(block * window, (block + 1) * window)
            for first in range(0, tile, window):
                rows = slice(first, first + window)
                value = dep_ref[part, block, rows, :]
                if block == 0:
                    value = value + left_ref[part, rows, :].astype(F32)
                if first == 0:
                    value = value + above_ref[part, block].astype(F32)
                out_ref[part, rows, cols] = (
                    upd_ref[part, block, rows, :] + value * den_ref[block, rows, :]
                )


VM = pl.BlockSpec(memory_space=pltpu.VMEM)
SM = pl.BlockSpec(memory_space=pltpu.SMEM)


def call(kernel, shapes, in_specs, scratch=(), name=None, flops=10**6):
    return pl.pallas_call(
        kernel,
        out_shape=[jax.ShapeDtypeStruct(shape, kind) for shape, kind in shapes],
        in_specs=in_specs,
        out_specs=[VM] * len(shapes),
        scratch_shapes=scratch,
        name=name,
        compiler_params=pltpu.CompilerParams(vmem_limit_bytes=40 * 2**20),
        cost_estimate=pl.CostEstimate(flops=flops, transcendentals=0, bytes_accessed=10**6),
    )


def exchange(parts, axis):
    return lax.all_to_all(parts, axis, 0, 0, tiled=True)


def on_device(object_field, probe, amplitude, corners, live_count):
    slots = amplitude.shape[2]
    window = probe.shape[1]
    tile = object_field.shape[1]
    wide = tile + window
    across = lax.axis_size("col")
    amp = amplitude.reshape(slots, window, window)
    spots = corners.reshape(2, slots)
    live = live_count.reshape(1, 1)
    tables = dft_tables(window)

    right = shift(object_field[:, :, :window].astype(HALO), "col", -1)
    low = shift(object_field[:, :window, :].astype(HALO), "row", -1)
    diagonal = shift(
        object_field[:, :window, :window].astype(HALO), ("row", "col"), -(across + 1)
    )
    scratch = [
        pltpu.VMEM((window, window), F32),
        pltpu.VMEM((GROUP, 2, window, window), F32),
        pltpu.VMEM((GROUP, window, 2 * window), BF16),
    ]
    ext, dep, to_right, to_left = call(
        first_kernel,
        [
            ((2, 3, wide, window), F32),
            ((3, 3, wide, window), F32),
            ((3, wide, window), TERMS),
            ((3, wide, window), TERMS),
        ],
        [SM, SM] + [VM] * 7,
        scratch,
        "first_sweep",
        10**9,
    )(live, spots, object_field, right, low, diagonal, probe, amp, tables)

    from_left = shift(to_right, "col", 1)
    from_right = shift(to_left, "col", -1)
    down, up = call(
        middle_kernel,
        [((3, 3, window, window), TERMS), ((3, 3, window, window), TERMS)],
        [VM] * 3,
        name="middle",
    )(dep, from_left, from_right)
    from_above = shift(down, "row", 1)
    from_below = shift(up, "row", -1)

    updated, inverse, dep, to_right, gradient = call(
        second_kernel,
        [
            ((2, 3, wide, window), F32),
            ((2, tile, window), F32),
            ((2, 3, wide, window), F32),
            ((2, wide, window), TERMS),
            ((2, window, window), F32),
        ],
        [SM, SM] + [VM] * 9,
        scratch,
        "second_sweep",
        10**9,
    )(live, spots, ext, dep, from_left, from_right, from_above, from_below, probe, amp, tables)

    rows, cols = lax.axis_size("row"), lax.axis_size("col")
    parts = exchange(gradient.astype(GRAD).reshape(rows, -1, window), "row")
    part = jnp.sum(parts.astype(F32), 0).astype(GRAD)
    to_right, dep, ignored = lax.optimization_barrier((to_right, dep, part))
    parts = exchange(jnp.broadcast_to(part[None], (cols,) + part.shape), "col")
    from_left = shift(to_right, "col", 1)
    spill = dep[:, :2, tile:, :]
    spill = jnp.concatenate(
        [(spill[:, :1] + from_left[:, None, tile:].astype(F32)), spill[:, 1:]], 1
    ).astype(TERMS)
    from_above = shift(spill, "row", 1)
    refined = call(
        finish_kernel, [((2, tile, tile), F32)], [VM] * 5, name="finish"
    )(updated, inverse, dep, from_left, from_above)[0]
    parts, refined = lax.optimization_barrier((parts, refined))
    part = jnp.sum(parts.astype(F32), 0)
    parts = exchange(jnp.broadcast_to(part[None], (rows,) + part.shape), "row")
    summed = parts.reshape(gradient.shape)
    spread = jnp.sqrt(jnp.mean(summed[0] * summed[0] + summed[1] * summed[1]) + 1e-06)
    new_probe = probe + summed / spread
    return (refined, new_probe)


def solution(mesh):
    in_specs = (
        P(None, "row", "col"),
        P(),
        P("row", "col", None, None, None),
        P(None, "row", "col", None),
        P("row", "col"),
    )
    out_specs = (P(None, "row", "col"), P())
    return jax.shard_map(
        on_device, mesh=mesh, in_specs=in_specs, out_specs=out_specs, check_vma=False
    )
```

```python
import functools
import math

import jax
import jax.numpy as jnp
import numpy as np
from jax import lax
from jax.experimental import pallas as pl
from jax.experimental.pallas import tpu as pltpu
from jax.sharding import PartitionSpec as P

GROUP = 8
F32 = jnp.float32
BF16 = jnp.bfloat16
HALO = BF16
TERMS = BF16
GRAD = BF16


def shift(value, axis, steps):
    count = lax.axis_size(axis)
    first, last = (max(0, -steps), min(count, count - steps))
    return lax.ppermute(value, axis, [(source, source + steps) for source in range(first, last)])


def dft_tables(window):
    indices = jnp.arange(window, dtype=jnp.int32)
    phase_index = indices[:, None] * indices[None, :] % window
    angles = phase_index.astype(F32) * (2.0 * math.pi / window)
    norming = 1.0 / math.sqrt(window)
    cosines = jnp.cos(angles) * norming
    sines = jnp.sin(angles) * norming
    turned = jnp.block([[cosines, sines], [-sines, cosines]])
    straight = jnp.block([[cosines, -sines], [sines, cosines]])
    return jnp.stack([straight, turned]).astype(BF16)


def dot(left, right):
    return lax.dot_general(left, right, (((1,), (0,)), ((), ())), preferred_element_type=F32)


def accumulate(ref, lead, block, row, turn, lanes, value):
    turned = pltpu.roll(value, turn, 1)
    window = value.shape[0]
    inner = lanes >= turn
    rows = pl.ds(row, window)
    ref[lead, block, rows, :] += jnp.where(inner, turned, 0.0)
    ref[lead, block + 1, rows, :] += jnp.where(inner, 0.0, turned)


def sweep_slots(
    live_ref, corners_ref, ext_ref, probe_ref, amp_ref, tab_ref,
    dep_ref, grad_ref, power_ref, patch_ref, wave_ref, with_light,
):
    window = probe_ref.shape[1]
    live = live_ref[0, 0]
    lanes = lax.broadcasted_iota(jnp.int32, (window, window), 1)
    straight = tab_ref[0]
    turned = tab_ref[1]

    def step(index, carry):
        base = index * GROUP
        spots = []
        waves = []
        for member in range(GROUP):
            slot = base + member
            row = corners_ref[0, slot]
            col = corners_ref[1, slot]
            block = col // window
            turn = col - block * window
            spots.append((slot, row, block, turn))
            back = jnp.where(turn == 0, 0, window - turn)
            inside = lanes < window - turn
            rows = pl.ds(row, window)
            pieces = []
            for part in range(2):
                near = pltpu.roll(ext_ref[part, block, rows, :], back, 1)
                far = pltpu.roll(ext_ref[part, block + 1, rows, :], back, 1)
                pieces.append(jnp.where(inside, near, far))
            if not with_light:
                patch_ref[member, 0] = pieces[0]
                patch_ref[member, 1] = pieces[1]
            pr, pi = probe_ref[0], probe_ref[1]
            real = (pr * pieces[0] - pi * pieces[1]).astype(BF16)
            imag = (pr * pieces[1] + pi * pieces[0]).astype(BF16)
            wave = jnp.concatenate([real, imag], 1)
            wave_ref[member] = wave
            waves.append(wave)
        pairs = [(m, m + 1) for m in range(0, GROUP, 2)]

        def beside(parts):
            return jnp.concatenate(
                [jnp.concatenate([h[:, :window], h[:, window:]], 0) for h in parts], 1
            )

        half = [[dot(waves[m], straight).astype(BF16) for m in ms] for ms in pairs]
        spectra = [dot(turned, beside(h)) for h in half]
        back = []
        for ms, spectrum in zip(pairs, spectra):
            projected = []
            for place, m in enumerate(ms):
                lo = place * window
                sr = spectrum[:window, lo : lo + window]
                si = spectrum[window:, lo : lo + window]
                amp = amp_ref[base + m].astype(F32)
                scale = amp * lax.rsqrt(jnp.maximum(sr * sr + si * si, 0.25))
                projected.append(
                    jnp.concatenate([(sr * scale).astype(BF16), (si * scale).astype(BF16)], 1)
                )
            back.append([dot(p, turned).astype(BF16) for p in projected])
        for ms, h in zip(pairs, back):
            returned = dot(straight, beside(h))
            for place, m in enumerate(ms):
                slot, row, block, turn = spots[m]
                weight = jnp.where(slot < live, 1.0, 0.0).astype(F32)
                lo = place * window
                wave = wave_ref[m].astype(F32)
                cr = (returned[:window, lo : lo + window] - wave[:, :window]) * weight
                ci = (returned[window:, lo : lo + window] - wave[:, window:]) * weight
                pr, pi = probe_ref[0], probe_ref[1]
                accumulate(dep_ref, 0, block, row, turn, lanes, pr * cr + pi * ci)
                accumulate(dep_ref, 1, block, row, turn, lanes, pr * ci - pi * cr)
                if with_light:
                    accumulate(dep_ref, 2, block, row, turn, lanes, power_ref[...] * weight)
                else:
                    xr, xi = patch_ref[m, 0], patch_ref[m, 1]
                    grad_ref[0] += xr * cr + xi * ci
                    grad_ref[1] += xr * ci - xi * cr
        return carry

    lax.fori_loop(0, (live + GROUP - 1) // GROUP, step, 0)


def first_kernel(
    live_ref, corners_ref, obj_ref, right_ref, low_ref, corner_ref, probe_ref, amp_ref, tab_ref,
    ext_ref, dep_ref, to_right_ref, to_left_ref, power_ref, patch_ref, wave_ref,
):
    window = probe_ref.shape[1]
    tile = obj_ref.shape[1]
    for part in range(2):
        for block in range(2):
            cols = slice(block * window, (block + 1) * window)
            ext_ref[part, block, 0:tile, :] = obj_ref[part, :, cols]
            ext_ref[part, block, tile:, :] = low_ref[part, :, cols].astype(F32)
        ext_ref[part, 2, 0:tile, :] = right_ref[part].astype(F32)
        ext_ref[part, 2, tile:, :] = corner_ref[part].astype(F32)
    dep_ref[...] = jnp.zeros(dep_ref.shape, F32)
    power_ref[...] = probe_ref[0] * probe_ref[0] + probe_ref[1] * probe_ref[1]
    sweep_slots(
        live_ref, corners_ref, ext_ref, probe_ref, amp_ref, tab_ref,
        dep_ref, None, power_ref, patch_ref, wave_ref, True,
    )
    for part in range(3):
        to_right_ref[part] = dep_ref[part, 2].astype(TERMS)
        to_left_ref[part] = dep_ref[part, 0].astype(TERMS)


def middle_kernel(dep_ref, from_left_ref, from_right_ref, down_ref, up_ref):
    window = from_left_ref.shape[2]
    tile = from_left_ref.shape[1] - window
    for part in range(3):
        for ref, rows in ((down_ref, slice(tile, tile + window)), (up_ref, slice(0, window))):
            ref[part, 0] = (dep_ref[part, 0, rows, :] + from_left_ref[part, rows, :].astype(F32)).astype(TERMS)
            ref[part, 1] = dep_ref[part, 1, rows, :].astype(TERMS)
            ref[part, 2] = (dep_ref[part, 2, rows, :] + from_right_ref[part, rows, :].astype(F32)).astype(TERMS)


def second_kernel(
    live_ref, corners_ref, ext_ref, dep_in_ref, left_ref, right_ref, above_ref, below_ref,
    probe_ref, amp_ref, tab_ref,
    upd_ref, den_ref, dep_ref, to_right_ref, grad_ref, sum_ref, patch_ref, wave_ref,
):
    window = probe_ref.shape[1]
    total = ext_ref.shape[2]
    tile = total - window
    for block in range(3):
        for first in range(0, total, window):
            rows = slice(first, first + window)
            sums = []
            for part in (2, 0, 1):
                value = dep_in_ref[part, block, rows, :]
                if block == 0:
                    value = value + left_ref[part, rows, :].astype(F32)
                if block == 2:
                    value = value + right_ref[part, rows, :].astype(F32)
                if first == 0:
                    value = value + above_ref[part, block].astype(F32)
                if first == tile:
                    value = value + below_ref[part, block].astype(F32)
                sums.append(value)
            inverse = 1.0 / (sums[0] + 4.0)
            for part in range(2):
                upd_ref[part, block, rows, :] = ext_ref[part, block, rows, :] + sums[part + 1] * inverse
            if first < tile and block < 2:
                den_ref[block, rows, :] = inverse
    dep_ref[...] = jnp.zeros(dep_ref.shape, F32)
    grad_ref[...] = jnp.zeros(grad_ref.shape, F32)
    sweep_slots(
        live_ref, corners_ref, upd_ref, probe_ref, amp_ref, tab_ref,
        dep_ref, grad_ref, None, patch_ref, wave_ref, False,
    )
    for part in range(2):
        to_right_ref[part] = dep_ref[part, 2].astype(TERMS)


def finish_kernel(upd_ref, den_ref, dep_ref, left_ref, above_ref, out_ref):
    window = left_ref.shape[2]
    tile = out_ref.shape[1]
    for part in range(2):
        for block in range(2):
            cols = slice(block * window, (block + 1) * window)
            for first in range(0, tile, window):
                rows = slice(first, first + window)
                value = dep_ref[part, block, rows, :]
                if block == 0:
                    value = value + left_ref[part, rows, :].astype(F32)
                if first == 0:
                    value = value + above_ref[part, block].astype(F32)
                out_ref[part, rows, cols] = (
                    upd_ref[part, block, rows, :] + value * den_ref[block, rows, :]
                )


VM = pl.BlockSpec(memory_space=pltpu.VMEM)
SM = pl.BlockSpec(memory_space=pltpu.SMEM)


def call(kernel, shapes, in_specs, scratch=(), name=None, flops=10**6):
    return pl.pallas_call(
        kernel,
        out_shape=[jax.ShapeDtypeStruct(shape, kind) for shape, kind in shapes],
        in_specs=in_specs,
        out_specs=[VM] * len(shapes),
        scratch_shapes=scratch,
        name=name,
        compiler_params=pltpu.CompilerParams(vmem_limit_bytes=40 * 2**20),
        cost_estimate=pl.CostEstimate(flops=flops, transcendentals=0, bytes_accessed=10**6),
    )


def exchange(parts, axis):
    return lax.all_to_all(parts, axis, 0, 0, tiled=True)


def on_device(object_field, probe, amplitude, corners, live_count):
    slots = amplitude.shape[2]
    window = probe.shape[1]
    tile = object_field.shape[1]
    wide = tile + window
    across = lax.axis_size("col")
    amp = amplitude.reshape(slots, window, window)
    spots = corners.reshape(2, slots)
    live = live_count.reshape(1, 1)
    tables = dft_tables(window)

    right = shift(object_field[:, :, :window].astype(HALO), "col", -1)
    low = shift(object_field[:, :window, :].astype(HALO), "row", -1)
    diagonal = shift(
        object_field[:, :window, :window].astype(HALO), ("row", "col"), -(across + 1)
    )
    scratch = [
        pltpu.VMEM((window, window), F32),
        pltpu.VMEM((GROUP, 2, window, window), F32),
        pltpu.VMEM((GROUP, window, 2 * window), BF16),
    ]
    ext, dep, to_right, to_left = call(
        first_kernel,
        [
            ((2, 3, wide, window), F32),
            ((3, 3, wide, window), F32),
            ((3, wide, window), TERMS),
            ((3, wide, window), TERMS),
        ],
        [SM, SM] + [VM] * 7,
        scratch,
        "first_sweep",
        10**9,
    )(live, spots, object_field, right, low, diagonal, probe, amp, tables)

    from_left = shift(to_right, "col", 1)
    from_right = shift(to_left, "col", -1)
    down, up = call(
        middle_kernel,
        [((3, 3, window, window), TERMS), ((3, 3, window, window), TERMS)],
        [VM] * 3,
        name="middle",
    )(dep, from_left, from_right)
    from_above = shift(down, "row", 1)
    from_below = shift(up, "row", -1)

    updated, inverse, dep, to_right, gradient = call(
        second_kernel,
        [
            ((2, 3, wide, window), F32),
            ((2, tile, window), F32),
            ((2, 3, wide, window), F32),
            ((2, wide, window), TERMS),
            ((2, window, window), F32),
        ],
        [SM, SM] + [VM] * 9,
        scratch,
        "second_sweep",
        10**9,
    )(live, spots, ext, dep, from_left, from_right, from_above, from_below, probe, amp, tables)

    rows, cols = lax.axis_size("row"), lax.axis_size("col")
    parts = exchange(gradient.astype(GRAD).reshape(rows, -1, window), "row")
    part = jnp.sum(parts.astype(F32), 0).astype(GRAD)
    to_right, dep, ignored = lax.optimization_barrier((to_right, dep, part))
    parts = exchange(jnp.broadcast_to(part[None], (cols,) + part.shape), "col")
    from_left = shift(to_right, "col", 1)
    spill = dep[:, :2, tile:, :]
    spill = jnp.concatenate(
        [(spill[:, :1] + from_left[:, None, tile:].astype(F32)), spill[:, 1:]], 1
    ).astype(TERMS)
    from_above = shift(spill, "row", 1)
    refined = call(
        finish_kernel, [((2, tile, tile), F32)], [VM] * 5, name="finish"
    )(updated, inverse, dep, from_left, from_above)[0]
    parts, refined = lax.optimization_barrier((parts, refined))
    part = jnp.sum(parts.astype(F32), 0)
    parts = exchange(jnp.broadcast_to(part[None], (rows,) + part.shape), "row")
    summed = parts.reshape(gradient.shape)
    spread = jnp.sqrt(jnp.mean(summed[0] * summed[0] + summed[1] * summed[1]) + 1e-06)
    new_probe = probe + summed / spread
    return (refined, new_probe)


def solution(mesh):
    in_specs = (
        P(None, "row", "col"),
        P(),
        P("row", "col", None, None, None),
        P(None, "row", "col", None),
        P("row", "col"),
    )
    out_specs = (P(None, "row", "col"), P())
    return jax.shard_map(
        on_device, mesh=mesh, in_specs=in_specs, out_specs=out_specs, check_vma=False
    )
```

```python
import math

import jax
import jax.numpy as jnp
from jax import lax
from jax.experimental import pallas as pl
from jax.experimental.pallas import tpu as pltpu
from jax.sharding import PartitionSpec as P


GROUP = 8
F32 = jnp.float32
BF16 = jnp.bfloat16
HALO = BF16
TERMS = BF16
GRAD = BF16


def shift(value, axis, steps):
    count = lax.axis_size(axis)
    first, last = (max(0, -steps), min(count, count - steps))
    return lax.ppermute(value, axis, [(source, source + steps) for source in range(first, last)])


def dft_tables(window):
    indices = jnp.arange(window, dtype=jnp.int32)
    phase_index = indices[:, None] * indices[None, :] % window
    angles = phase_index.astype(F32) * (2.0 * math.pi / window)
    norming = 1.0 / math.sqrt(window)
    cosines = jnp.cos(angles) * norming
    sines = jnp.sin(angles) * norming
    turned = jnp.block([[cosines, sines], [-sines, cosines]])
    straight = jnp.block([[cosines, -sines], [sines, cosines]])
    return jnp.stack([straight, turned]).astype(BF16)


def dot(left, right):
    return lax.dot_general(left, right, (((1,), (0,)), ((), ())), preferred_element_type=F32)


def accumulate(ref, lead, block, row, turn, lanes, value):
    turned = pltpu.roll(value, turn, 1)
    window = value.shape[0]
    inner = lanes >= turn
    rows = pl.ds(row, window)
    ref[lead, block, rows, :] += jnp.where(inner, turned, 0.0)
    ref[lead, block + 1, rows, :] += jnp.where(inner, 0.0, turned)


def sweep_slots(
    live_ref, corners_ref, ext_ref, probe_ref, amp_ref, tab_ref,
    dep_ref, grad_ref, power_ref, patch_ref, wave_ref, with_light,
):
    window = probe_ref.shape[1]
    live = live_ref[0, 0]
    lanes = lax.broadcasted_iota(jnp.int32, (window, window), 1)
    straight = tab_ref[0]
    turned = tab_ref[1]

    def step(index, carry):
        base = index * GROUP
        spots = []
        waves = []
        for member in range(GROUP):
            slot = base + member
            row = corners_ref[0, slot]
            col = corners_ref[1, slot]
            block = col // window
            turn = col - block * window
            spots.append((slot, row, block, turn))
            back = jnp.where(turn == 0, 0, window - turn)
            inside = lanes < window - turn
            rows = pl.ds(row, window)
            pieces = []
            for part in range(2):
                near = pltpu.roll(ext_ref[part, block, rows, :], back, 1)
                far = pltpu.roll(ext_ref[part, block + 1, rows, :], back, 1)
                pieces.append(jnp.where(inside, near, far))
            if not with_light:
                patch_ref[member, 0] = pieces[0]
                patch_ref[member, 1] = pieces[1]
            pr, pi = probe_ref[0], probe_ref[1]
            real = (pr * pieces[0] - pi * pieces[1]).astype(BF16)
            imag = (pr * pieces[1] + pi * pieces[0]).astype(BF16)
            wave = jnp.concatenate([real, imag], 1)
            wave_ref[member] = wave
            waves.append(wave)
        pairs = [(m, m + 1) for m in range(0, GROUP, 2)]

        def beside(parts):
            return jnp.concatenate(
                [jnp.concatenate([h[:, :window], h[:, window:]], 0) for h in parts], 1
            )

        half = [[dot(waves[m], straight).astype(BF16) for m in ms] for ms in pairs]
        spectra = [dot(turned, beside(h)) for h in half]
        back = []
        for ms, spectrum in zip(pairs, spectra):
            projected = []
            for place, m in enumerate(ms):
                lo = place * window
                sr = spectrum[:window, lo : lo + window]
                si = spectrum[window:, lo : lo + window]
                amp = amp_ref[base + m].astype(F32)
                scale = amp * lax.rsqrt(jnp.maximum(sr * sr + si * si, 0.25))
                projected.append(
                    jnp.concatenate([(sr * scale).astype(BF16), (si * scale).astype(BF16)], 1)
                )
            back.append([dot(p, turned).astype(BF16) for p in projected])
        for ms, h in zip(pairs, back):
            returned = dot(straight, beside(h))
            for place, m in enumerate(ms):
                slot, row, block, turn = spots[m]
                weight = jnp.where(slot < live, 1.0, 0.0).astype(F32)
                lo = place * window
                wave = wave_ref[m].astype(F32)
                cr = (returned[:window, lo : lo + window] - wave[:, :window]) * weight
                ci = (returned[window:, lo : lo + window] - wave[:, window:]) * weight
                pr, pi = probe_ref[0], probe_ref[1]
                accumulate(dep_ref, 0, block, row, turn, lanes, pr * cr + pi * ci)
                accumulate(dep_ref, 1, block, row, turn, lanes, pr * ci - pi * cr)
                if with_light:
                    accumulate(dep_ref, 2, block, row, turn, lanes, power_ref[...] * weight)
                else:
                    xr, xi = patch_ref[m, 0], patch_ref[m, 1]
                    grad_ref[0] += xr * cr + xi * ci
                    grad_ref[1] += xr * ci - xi * cr
        return carry

    lax.fori_loop(0, (live + GROUP - 1) // GROUP, step, 0)


def first_kernel(
    live_ref, corners_ref, obj_ref, right_ref, low_ref, corner_ref, probe_ref, amp_ref, tab_ref,
    ext_ref, dep_ref, to_right_ref, to_left_ref, power_ref, patch_ref, wave_ref,
):
    window = probe_ref.shape[1]
    tile = obj_ref.shape[1]
    for part in range(2):
        for block in range(2):
            cols = slice(block * window, (block + 1) * window)
            ext_ref[part, block, 0:tile, :] = obj_ref[part, :, cols]
            ext_ref[part, block, tile:, :] = low_ref[part, :, cols].astype(F32)
        ext_ref[part, 2, 0:tile, :] = right_ref[part].astype(F32)
        ext_ref[part, 2, tile:, :] = corner_ref[part].astype(F32)
    dep_ref[...] = jnp.zeros(dep_ref.shape, F32)
    power_ref[...] = probe_ref[0] * probe_ref[0] + probe_ref[1] * probe_ref[1]
    sweep_slots(
        live_ref, corners_ref, ext_ref, probe_ref, amp_ref, tab_ref,
        dep_ref, None, power_ref, patch_ref, wave_ref, True,
    )
    for part in range(3):
        to_right_ref[part] = dep_ref[part, 2].astype(TERMS)
        to_left_ref[part] = dep_ref[part, 0].astype(TERMS)


def middle_kernel(dep_ref, from_left_ref, from_right_ref, down_ref, up_ref):
    window = from_left_ref.shape[2]
    tile = from_left_ref.shape[1] - window
    for part in range(3):
        for ref, rows in ((down_ref, slice(tile, tile + window)), (up_ref, slice(0, window))):
            ref[part, 0] = (dep_ref[part, 0, rows, :] + from_left_ref[part, rows, :].astype(F32)).astype(TERMS)
            ref[part, 1] = dep_ref[part, 1, rows, :].astype(TERMS)
            ref[part, 2] = (dep_ref[part, 2, rows, :] + from_right_ref[part, rows, :].astype(F32)).astype(TERMS)


def second_kernel(
    live_ref, corners_ref, ext_ref, dep_in_ref, left_ref, right_ref, above_ref, below_ref,
    probe_ref, amp_ref, tab_ref,
    upd_ref, den_ref, dep_ref, to_right_ref, grad_ref, sum_ref, patch_ref, wave_ref,
):
    window = probe_ref.shape[1]
    total = ext_ref.shape[2]
    tile = total - window
    for block in range(3):
        for first in range(0, total, window):
            rows = slice(first, first + window)
            sums = []
            for part in (2, 0, 1):
                value = dep_in_ref[part, block, rows, :]
                if block == 0:
                    value = value + left_ref[part, rows, :].astype(F32)
                if block == 2:
                    value = value + right_ref[part, rows, :].astype(F32)
                if first == 0:
                    value = value + above_ref[part, block].astype(F32)
                if first == tile:
                    value = value + below_ref[part, block].astype(F32)
                sums.append(value)
            inverse = 1.0 / (sums[0] + 4.0)
            for part in range(2):
                upd_ref[part, block, rows, :] = ext_ref[part, block, rows, :] + sums[part + 1] * inverse
            if first < tile and block < 2:
                den_ref[block, rows, :] = inverse
    dep_ref[...] = jnp.zeros(dep_ref.shape, F32)
    grad_ref[...] = jnp.zeros(grad_ref.shape, F32)
    sweep_slots(
        live_ref, corners_ref, upd_ref, probe_ref, amp_ref, tab_ref,
        dep_ref, grad_ref, None, patch_ref, wave_ref, False,
    )
    for part in range(2):
        to_right_ref[part] = dep_ref[part, 2].astype(TERMS)


def finish_kernel(upd_ref, den_ref, dep_ref, left_ref, above_ref, out_ref):
    window = left_ref.shape[2]
    tile = out_ref.shape[1]
    for part in range(2):
        for block in range(2):
            cols = slice(block * window, (block + 1) * window)
            for first in range(0, tile, window):
                rows = slice(first, first + window)
                value = dep_ref[part, block, rows, :]
                if block == 0:
                    value = value + left_ref[part, rows, :].astype(F32)
                if first == 0:
                    value = value + above_ref[part, block].astype(F32)
                out_ref[part, rows, cols] = (
                    upd_ref[part, block, rows, :] + value * den_ref[block, rows, :]
                )


def probe_kernel(probe_ref, sum_ref, out_ref):
    summed = sum_ref[...]
    power = jnp.sum(summed * summed, axis=(0, 1, 2), keepdims=True)
    scale = 1.0 / jnp.sqrt(power / (out_ref.shape[1] * out_ref.shape[2]) + 1e-06)
    out_ref[...] = probe_ref[...] + summed * scale


VM = pl.BlockSpec(memory_space=pltpu.VMEM)
SM = pl.BlockSpec(memory_space=pltpu.SMEM)


def call(kernel, shapes, in_specs, scratch=(), flops=10**6):
    return pl.pallas_call(
        kernel,
        out_shape=[jax.ShapeDtypeStruct(shape, kind) for shape, kind in shapes],
        in_specs=in_specs,
        out_specs=[VM] * len(shapes),
        scratch_shapes=scratch,
        compiler_params=pltpu.CompilerParams(vmem_limit_bytes=40 * 2**20),
        cost_estimate=pl.CostEstimate(flops=flops, transcendentals=0, bytes_accessed=10**6),
    )


def exchange(parts, axis):
    return lax.all_to_all(parts, axis, 0, 0, tiled=True)


def sweeps(object_field, probe, amplitude, corners, live_count):
    slots = amplitude.shape[2]
    window = probe.shape[1]
    tile = object_field.shape[1]
    wide = tile + window
    across = lax.axis_size("col")
    amp = amplitude.reshape(slots, window, window)
    spots = corners.reshape(2, slots)
    live = live_count.reshape(1, 1)
    tables = dft_tables(window)

    right = shift(object_field[:, :, :window].astype(HALO), "col", -1)
    low = shift(object_field[:, :window, :].astype(HALO), "row", -1)
    diagonal = shift(
        object_field[:, :window, :window].astype(HALO), ("row", "col"), -(across + 1)
    )
    scratch = [
        pltpu.VMEM((window, window), F32),
        pltpu.VMEM((GROUP, 2, window, window), F32),
        pltpu.VMEM((GROUP, window, 2 * window), BF16),
    ]
    ext, dep, to_right, to_left = call(
        first_kernel,
        [
            ((2, 3, wide, window), F32),
            ((3, 3, wide, window), F32),
            ((3, wide, window), TERMS),
            ((3, wide, window), TERMS),
        ],
        [SM, SM] + [VM] * 7,
        scratch,
        10**9,
    )(live, spots, object_field, right, low, diagonal, probe, amp, tables)

    from_left = shift(to_right, "col", 1)
    from_right = shift(to_left, "col", -1)
    down, up = call(
        middle_kernel, [((3, 3, window, window), TERMS), ((3, 3, window, window), TERMS)], [VM] * 3
    )(dep, from_left, from_right)
    from_above = shift(down, "row", 1)
    from_below = shift(up, "row", -1)

    updated, inverse, dep, to_right, gradient = call(
        second_kernel,
        [
            ((2, 3, wide, window), F32),
            ((2, tile, window), F32),
            ((2, 3, wide, window), F32),
            ((2, wide, window), TERMS),
            ((2, window, window), F32),
        ],
        [SM, SM] + [VM] * 9,
        scratch,
        10**9,
    )(live, spots, ext, dep, from_left, from_right, from_above, from_below, probe, amp, tables)

    rows, cols = lax.axis_size("row"), lax.axis_size("col")
    parts = exchange(gradient.astype(GRAD).reshape(rows, -1, window), "row")
    part = jnp.sum(parts.astype(F32), 0).astype(GRAD)
    to_right, dep, ignored = lax.optimization_barrier((to_right, dep, part))
    parts = exchange(jnp.broadcast_to(part[None], (cols,) + part.shape), "col")
    from_left = shift(to_right, "col", 1)
    spill = dep[:, :2, tile:, :]
    spill = jnp.concatenate(
        [(spill[:, :1] + from_left[:, None, tile:].astype(F32)), spill[:, 1:]], 1
    ).astype(TERMS)
    part = jnp.sum(parts.astype(F32), 0)
    spill, ignored = lax.optimization_barrier((spill, part))
    parts = exchange(jnp.broadcast_to(part[None], (rows,) + part.shape), "row")
    from_above = shift(spill, "row", 1)
    refined = call(
        finish_kernel, [((2, tile, tile), F32)], [VM] * 5
    )(updated, inverse, dep, from_left, from_above)[0]
    new_probe = call(probe_kernel, [(probe.shape, F32)], [VM] * 2)(
        probe, parts.reshape(gradient.shape)
    )[0]
    return (refined, new_probe)


def solution(mesh):
    in_specs = (
        P(None, "row", "col"),
        P(),
        P("row", "col", None, None, None),
        P(None, "row", "col", None),
        P("row", "col"),
    )
    out_specs = (P(None, "row", "col"), P())
    return jax.shard_map(sweeps, mesh=mesh, in_specs=in_specs, out_specs=out_specs, check_vma=False)
```

```python
import math

import jax
import jax.numpy as jnp
from jax import lax
from jax.experimental import pallas as pl
from jax.experimental.pallas import tpu as pltpu
from jax.sharding import PartitionSpec as P


GROUP = 8
F32 = jnp.float32
BF16 = jnp.bfloat16
HALO = BF16
TERMS = BF16
GRAD = BF16


def shift(value, axis, steps):
    count = lax.axis_size(axis)
    first, last = (max(0, -steps), min(count, count - steps))
    return lax.ppermute(value, axis, [(source, source + steps) for source in range(first, last)])


def dft_tables(window):
    indices = jnp.arange(window, dtype=jnp.int32)
    phase_index = indices[:, None] * indices[None, :] % window
    angles = phase_index.astype(F32) * (2.0 * math.pi / window)
    norming = 1.0 / math.sqrt(window)
    cosines = jnp.cos(angles) * norming
    sines = jnp.sin(angles) * norming
    turned = jnp.block([[cosines, sines], [-sines, cosines]])
    straight = jnp.block([[cosines, -sines], [sines, cosines]])
    return jnp.stack([straight, turned]).astype(BF16)


def dot(left, right):
    return lax.dot_general(left, right, (((1,), (0,)), ((), ())), preferred_element_type=F32)


def accumulate(ref, lead, block, row, turn, lanes, value):
    turned = pltpu.roll(value, turn, 1)
    window = value.shape[0]
    inner = lanes >= turn
    rows = pl.ds(row, window)
    ref[lead, block, rows, :] += jnp.where(inner, turned, 0.0)
    ref[lead, block + 1, rows, :] += jnp.where(inner, 0.0, turned)


def sweep_slots(
    live_ref, corners_ref, ext_ref, probe_ref, amp_ref, tab_ref,
    dep_ref, grad_ref, patch_ref, wave_ref,
):
    window = probe_ref.shape[1]
    live = live_ref[0, 0]
    lanes = lax.broadcasted_iota(jnp.int32, (window, window), 1)
    straight = tab_ref[0]
    turned = tab_ref[1]

    def step(index, carry):
        base = index * GROUP
        spots = []
        waves = []
        for member in range(GROUP):
            slot = base + member
            row = corners_ref[0, slot]
            col = corners_ref[1, slot]
            block = col // window
            turn = col - block * window
            spots.append((slot, row, block, turn))
            back = jnp.where(turn == 0, 0, window - turn)
            inside = lanes < window - turn
            rows = pl.ds(row, window)
            pieces = []
            for part in range(2):
                near = pltpu.roll(ext_ref[part, block, rows, :], back, 1)
                far = pltpu.roll(ext_ref[part, block + 1, rows, :], back, 1)
                pieces.append(jnp.where(inside, near, far))
            if grad_ref is not None:
                patch_ref[member, 0] = pieces[0]
                patch_ref[member, 1] = pieces[1]
            pr, pi = probe_ref[0], probe_ref[1]
            real = (pr * pieces[0] - pi * pieces[1]).astype(BF16)
            imag = (pr * pieces[1] + pi * pieces[0]).astype(BF16)
            wave = jnp.concatenate([real, imag], 1)
            wave_ref[member] = wave
            waves.append(wave)
        pairs = [(m, m + 1) for m in range(0, GROUP, 2)]

        def beside(parts):
            return jnp.concatenate(
                [jnp.concatenate([h[:, :window], h[:, window:]], 0) for h in parts], 1
            )

        half = [[dot(waves[m], straight).astype(BF16) for m in ms] for ms in pairs]
        spectra = [dot(turned, beside(h)) for h in half]
        back = []
        for ms, spectrum in zip(pairs, spectra):
            projected = []
            for place, m in enumerate(ms):
                lo = place * window
                sr = spectrum[:window, lo : lo + window]
                si = spectrum[window:, lo : lo + window]
                amp = amp_ref[base + m].astype(F32)
                scale = amp * lax.rsqrt(jnp.maximum(sr * sr + si * si, 0.25))
                projected.append(
                    jnp.concatenate([(sr * scale).astype(BF16), (si * scale).astype(BF16)], 1)
                )
            back.append([dot(p, turned).astype(BF16) for p in projected])
        for ms, h in zip(pairs, back):
            returned = dot(straight, beside(h))
            for place, m in enumerate(ms):
                slot, row, block, turn = spots[m]
                weight = jnp.where(slot < live, 1.0, 0.0).astype(F32)
                lo = place * window
                wave = wave_ref[m].astype(F32)
                cr = (returned[:window, lo : lo + window] - wave[:, :window]) * weight
                ci = (returned[window:, lo : lo + window] - wave[:, window:]) * weight
                pr, pi = probe_ref[0], probe_ref[1]
                accumulate(dep_ref, 0, block, row, turn, lanes, pr * cr + pi * ci)
                accumulate(dep_ref, 1, block, row, turn, lanes, pr * ci - pi * cr)
                if grad_ref is not None:
                    xr, xi = patch_ref[m, 0], patch_ref[m, 1]
                    grad_ref[0] += xr * cr + xi * ci
                    grad_ref[1] += xr * ci - xi * cr
        return carry

    lax.fori_loop(0, (live + GROUP - 1) // GROUP, step, 0)


def light_kernel(
    live_ref, corners_ref, probe_ref, light_ref, to_right_ref, to_left_ref, power_ref
):
    window = probe_ref.shape[1]
    live = live_ref[0, 0]
    lanes = lax.broadcasted_iota(jnp.int32, (window, window), 1)
    light_ref[...] = jnp.zeros(light_ref.shape, F32)
    power_ref[...] = probe_ref[0] * probe_ref[0] + probe_ref[1] * probe_ref[1]

    def step(index, carry):
        for member in range(4):
            slot = index * 4 + member
            weight = jnp.where(slot < live, 1.0, 0.0).astype(F32)
            row = corners_ref[0, slot]
            col = corners_ref[1, slot]
            block = col // window
            accumulate(
                light_ref, 0, block, row, col - block * window, lanes, power_ref[...] * weight
            )
        return carry

    lax.fori_loop(0, (live + 3) // 4, step, 0)
    to_right_ref[0] = light_ref[0, 2].astype(TERMS)
    to_left_ref[0] = light_ref[0, 0].astype(TERMS)


def first_kernel(
    live_ref, corners_ref, obj_ref, right_ref, low_ref, corner_ref, probe_ref, amp_ref, tab_ref,
    ext_ref, dep_ref, to_right_ref, to_left_ref, patch_ref, wave_ref,
):
    window = probe_ref.shape[1]
    tile = obj_ref.shape[1]
    for part in range(2):
        for block in range(2):
            cols = slice(block * window, (block + 1) * window)
            ext_ref[part, block, 0:tile, :] = obj_ref[part, :, cols]
            ext_ref[part, block, tile:, :] = low_ref[part, :, cols].astype(F32)
        ext_ref[part, 2, 0:tile, :] = right_ref[part].astype(F32)
        ext_ref[part, 2, tile:, :] = corner_ref[part].astype(F32)
    dep_ref[...] = jnp.zeros(dep_ref.shape, F32)
    sweep_slots(
        live_ref, corners_ref, ext_ref, probe_ref, amp_ref, tab_ref,
        dep_ref, None, patch_ref, wave_ref,
    )
    for part in range(2):
        to_right_ref[part] = dep_ref[part, 2].astype(TERMS)
        to_left_ref[part] = dep_ref[part, 0].astype(TERMS)


def middle_kernel(
    dep_ref, light_ref, from_left_ref, from_right_ref, light_left_ref, light_right_ref,
    down_ref, up_ref,
):
    window = from_left_ref.shape[2]
    tile = from_left_ref.shape[1] - window
    sources = [(dep_ref, from_left_ref, from_right_ref, part, part) for part in range(2)]
    sources.append((light_ref, light_left_ref, light_right_ref, 0, 2))
    for own, left, right, part, place in sources:
        for ref, rows in ((down_ref, slice(tile, tile + window)), (up_ref, slice(0, window))):
            ref[place, 0] = (own[part, 0, rows, :] + left[part, rows, :].astype(F32)).astype(TERMS)
            ref[place, 1] = own[part, 1, rows, :].astype(TERMS)
            ref[place, 2] = (own[part, 2, rows, :] + right[part, rows, :].astype(F32)).astype(TERMS)


def second_kernel(
    live_ref, corners_ref, ext_ref, dep_in_ref, light_ref, left_ref, right_ref,
    light_left_ref, light_right_ref, above_ref, below_ref,
    probe_ref, amp_ref, tab_ref,
    upd_ref, den_ref, dep_ref, to_right_ref, grad_ref, patch_ref, wave_ref,
):
    window = probe_ref.shape[1]
    total = ext_ref.shape[2]
    tile = total - window
    for block in range(3):
        for first in range(0, total, window):
            rows = slice(first, first + window)
            sums = []
            for part in (2, 0, 1):
                own, left, right, place = dep_in_ref, left_ref, right_ref, part
                if part == 2:
                    own, left, right, place = light_ref, light_left_ref, light_right_ref, 0
                value = own[place, block, rows, :]
                if block == 0:
                    value = value + left[place, rows, :].astype(F32)
                if block == 2:
                    value = value + right[place, rows, :].astype(F32)
                if first == 0:
                    value = value + above_ref[part, block].astype(F32)
                if first == tile:
                    value = value + below_ref[part, block].astype(F32)
                sums.append(value)
            inverse = 1.0 / (sums[0] + 4.0)
            for part in range(2):
                upd_ref[part, block, rows, :] = ext_ref[part, block, rows, :] + sums[part + 1] * inverse
            if first < tile and block < 2:
                den_ref[block, rows, :] = inverse
    dep_ref[...] = jnp.zeros(dep_ref.shape, F32)
    grad_ref[...] = jnp.zeros(grad_ref.shape, F32)
    sweep_slots(
        live_ref, corners_ref, upd_ref, probe_ref, amp_ref, tab_ref,
        dep_ref, grad_ref, patch_ref, wave_ref,
    )
    for part in range(2):
        to_right_ref[part] = dep_ref[part, 2].astype(TERMS)


def finish_kernel(upd_ref, den_ref, dep_ref, left_ref, above_ref, out_ref):
    window = left_ref.shape[2]
    tile = out_ref.shape[1]
    for part in range(2):
        for block in range(2):
            cols = slice(block * window, (block + 1) * window)
            for first in range(0, tile, window):
                rows = slice(first, first + window)
                value = dep_ref[part, block, rows, :]
                if block == 0:
                    value = value + left_ref[part, rows, :].astype(F32)
                if first == 0:
                    value = value + above_ref[part, block].astype(F32)
                out_ref[part, rows, cols] = (
                    upd_ref[part, block, rows, :] + value * den_ref[block, rows, :]
                )


def probe_kernel(probe_ref, sum_ref, out_ref):
    summed = sum_ref[...]
    power = jnp.sum(summed * summed, axis=(0, 1, 2), keepdims=True)
    scale = 1.0 / jnp.sqrt(power / (out_ref.shape[1] * out_ref.shape[2]) + 1e-06)
    out_ref[...] = probe_ref[...] + summed * scale


VM = pl.BlockSpec(memory_space=pltpu.VMEM)
SM = pl.BlockSpec(memory_space=pltpu.SMEM)


def call(kernel, shapes, in_specs, scratch=(), flops=10**6):
    return pl.pallas_call(
        kernel,
        out_shape=[jax.ShapeDtypeStruct(shape, kind) for shape, kind in shapes],
        in_specs=in_specs,
        out_specs=[VM] * len(shapes),
        scratch_shapes=scratch,
        compiler_params=pltpu.CompilerParams(vmem_limit_bytes=40 * 2**20),
        cost_estimate=pl.CostEstimate(flops=flops, transcendentals=0, bytes_accessed=10**6),
    )


def exchange(parts, axis):
    return lax.all_to_all(parts, axis, 0, 0, tiled=True)


def sweeps(object_field, probe, amplitude, corners, live_count):
    slots = amplitude.shape[2]
    window = probe.shape[1]
    tile = object_field.shape[1]
    wide = tile + window

    amp = amplitude.reshape(slots, window, window)
    spots = corners.reshape(2, slots)
    live = live_count.reshape(1, 1)
    tables = dft_tables(window)

    diagonal = shift(
        object_field[:, :window, :window].astype(HALO), ("row", "col"), -(lax.axis_size("col") + 1)
    )
    right = shift(object_field[:, :, :window].astype(HALO), "col", -1)
    low = shift(object_field[:, :window, :].astype(HALO), "row", -1)
    strip = (wide, window)
    light, light_right, light_left = call(
        light_kernel,
        [((1, 3) + strip, F32), ((1,) + strip, TERMS), ((1,) + strip, TERMS)],
        [SM, SM, VM],
        [pltpu.VMEM((window, window), F32)],
    )(live, spots, probe)
    light_from_left = shift(light_right, "col", 1)
    light_from_right = shift(light_left, "col", -1)
    scratch = [
        pltpu.VMEM((GROUP, 2, window, window), F32),
        pltpu.VMEM((GROUP, window, 2 * window), BF16),
    ]
    ext, dep, to_right, to_left = call(
        first_kernel,
        [
            ((2, 3) + strip, F32),
            ((2, 3) + strip, F32),
            ((2,) + strip, TERMS),
            ((2,) + strip, TERMS),
        ],
        [SM, SM] + [VM] * 7,
        scratch,
        10**9,
    )(live, spots, object_field, right, low, diagonal, probe, amp, tables)

    from_left = shift(to_right, "col", 1)
    from_right = shift(to_left, "col", -1)
    down, up = call(
        middle_kernel, [((3, 3, window, window), TERMS), ((3, 3, window, window), TERMS)], [VM] * 6
    )(dep, light, from_left, from_right, light_from_left, light_from_right)
    from_above = shift(down, "row", 1)
    from_below = shift(up, "row", -1)

    updated, inverse, dep, to_right, gradient = call(
        second_kernel,
        [
            ((2, 3, wide, window), F32),
            ((2, tile, window), F32),
            ((2, 3, wide, window), F32),
            ((2, wide, window), TERMS),
            ((2, window, window), F32),
        ],
        [SM, SM] + [VM] * 12,
        scratch,
        10**9,
    )(
        live, spots, ext, dep, light, from_left, from_right, light_from_left, light_from_right,
        from_above, from_below, probe, amp, tables,
    )

    rows, cols = lax.axis_size("row"), lax.axis_size("col")
    parts = exchange(gradient.astype(GRAD).reshape(rows, -1, window), "row")
    part = jnp.sum(parts.astype(F32), 0).astype(GRAD)
    to_right, dep, _ = lax.optimization_barrier((to_right, dep, part))
    parts = exchange(jnp.broadcast_to(part[None], (cols,) + part.shape), "col")
    from_left = shift(to_right, "col", 1)
    spill = dep[:, :2, tile:, :]
    spill = jnp.concatenate(
        [(spill[:, :1] + from_left[:, None, tile:].astype(F32)), spill[:, 1:]], 1
    ).astype(TERMS)
    from_above = shift(spill, "row", 1)
    refined = call(
        finish_kernel, [((2, tile, tile), F32)], [VM] * 5
    )(updated, inverse, dep, from_left, from_above)[0]
    parts, refined = lax.optimization_barrier((parts, refined))
    part = jnp.sum(parts.astype(F32), 0)
    parts = exchange(jnp.broadcast_to(part[None], (rows,) + part.shape), "row")
    new_probe = call(probe_kernel, [(probe.shape, F32)], [VM] * 2)(
        probe, parts.reshape(gradient.shape)
    )[0]
    return (refined, new_probe)


def solution(mesh):
    in_specs = (
        P(None, "row", "col"),
        P(),
        P("row", "col", None, None, None),
        P(None, "row", "col", None),
        P("row", "col"),
    )
    out_specs = (P(None, "row", "col"), P())
    return jax.shard_map(sweeps, mesh=mesh, in_specs=in_specs, out_specs=out_specs, check_vma=False)
```

```python
import math

import jax
import jax.numpy as jnp
from jax import lax
from jax.experimental import pallas as pl
from jax.experimental.pallas import tpu as pltpu
from jax.sharding import PartitionSpec as P


GROUP = 8
F32 = jnp.float32
BF16 = jnp.bfloat16
HALO = BF16
TERMS = BF16
GRAD = BF16


def shift(value, axis, steps):
    count = lax.axis_size(axis)
    first, last = (max(0, -steps), min(count, count - steps))
    return lax.ppermute(value, axis, [(source, source + steps) for source in range(first, last)])


def dft_tables(window):
    indices = jnp.arange(window, dtype=jnp.int32)
    phase_index = indices[:, None] * indices[None, :] % window
    angles = phase_index.astype(F32) * (2.0 * math.pi / window)
    norming = 1.0 / math.sqrt(window)
    cosines = jnp.cos(angles) * norming
    sines = jnp.sin(angles) * norming
    turned = jnp.block([[cosines, sines], [-sines, cosines]])
    straight = jnp.block([[cosines, -sines], [sines, cosines]])
    return jnp.stack([straight, turned]).astype(BF16)


def dot(left, right):
    return lax.dot_general(left, right, (((1,), (0,)), ((), ())), preferred_element_type=F32)


def accumulate(ref, lead, block, row, turn, lanes, value):
    turned = pltpu.roll(value, turn, 1)
    window = value.shape[0]
    inner = lanes >= turn
    rows = pl.ds(row, window)
    ref[lead, block, rows, :] += jnp.where(inner, turned, 0.0)
    ref[lead, block + 1, rows, :] += jnp.where(inner, 0.0, turned)


def sweep_slots(
    live_ref, corners_ref, ext_ref, probe_ref, amp_ref, tab_ref,
    dep_ref, grad_ref, power_ref, patch_ref, wave_ref, with_light,
):
    window = probe_ref.shape[1]
    live = live_ref[0, 0]
    lanes = lax.broadcasted_iota(jnp.int32, (window, window), 1)
    straight = tab_ref[0]
    turned = tab_ref[1]

    def step(index, carry):
        base = index * GROUP
        spots = []
        waves = []
        for member in range(GROUP):
            slot = base + member
            row = corners_ref[0, slot]
            col = corners_ref[1, slot]
            block = col // window
            turn = col - block * window
            spots.append((slot, row, block, turn))
            back = jnp.where(turn == 0, 0, window - turn)
            inside = lanes < window - turn
            rows = pl.ds(row, window)
            pieces = []
            for part in range(2):
                near = pltpu.roll(ext_ref[part, block, rows, :], back, 1)
                far = pltpu.roll(ext_ref[part, block + 1, rows, :], back, 1)
                pieces.append(jnp.where(inside, near, far))
            if not with_light:
                patch_ref[member, 0] = pieces[0]
                patch_ref[member, 1] = pieces[1]
            pr, pi = probe_ref[0], probe_ref[1]
            real = (pr * pieces[0] - pi * pieces[1]).astype(BF16)
            imag = (pr * pieces[1] + pi * pieces[0]).astype(BF16)
            wave = jnp.concatenate([real, imag], 1)
            wave_ref[member] = wave
            waves.append(wave)
        pairs = [(m, m + 1) for m in range(0, GROUP, 2)]

        def beside(parts):
            return jnp.concatenate(
                [jnp.concatenate([h[:, :window], h[:, window:]], 0) for h in parts], 1
            )

        half = [[dot(waves[m], straight).astype(BF16) for m in ms] for ms in pairs]
        spectra = [dot(turned, beside(h)) for h in half]
        back = []
        for ms, spectrum in zip(pairs, spectra):
            projected = []
            for place, m in enumerate(ms):
                lo = place * window
                sr = spectrum[:window, lo : lo + window]
                si = spectrum[window:, lo : lo + window]
                amp = amp_ref[base + m].astype(F32)
                scale = amp * lax.rsqrt(jnp.maximum(sr * sr + si * si, 0.25))
                projected.append(
                    jnp.concatenate([(sr * scale).astype(BF16), (si * scale).astype(BF16)], 1)
                )
            back.append([dot(p, turned).astype(BF16) for p in projected])
        for ms, h in zip(pairs, back):
            returned = dot(straight, beside(h))
            for place, m in enumerate(ms):
                slot, row, block, turn = spots[m]
                weight = jnp.where(slot < live, 1.0, 0.0).astype(F32)
                lo = place * window
                wave = wave_ref[m].astype(F32)
                cr = (returned[:window, lo : lo + window] - wave[:, :window]) * weight
                ci = (returned[window:, lo : lo + window] - wave[:, window:]) * weight
                pr, pi = probe_ref[0], probe_ref[1]
                accumulate(dep_ref, 0, block, row, turn, lanes, pr * cr + pi * ci)
                accumulate(dep_ref, 1, block, row, turn, lanes, pr * ci - pi * cr)
                if with_light:
                    accumulate(dep_ref, 2, block, row, turn, lanes, power_ref[...] * weight)
                else:
                    xr, xi = patch_ref[m, 0], patch_ref[m, 1]
                    grad_ref[0] += xr * cr + xi * ci
                    grad_ref[1] += xr * ci - xi * cr
        return carry

    lax.fori_loop(0, (live + GROUP - 1) // GROUP, step, 0)


def first_kernel(
    live_ref, corners_ref, obj_ref, right_ref, low_ref, corner_ref, probe_ref, amp_ref, tab_ref,
    ext_ref, dep_ref, to_right_ref, to_left_ref, power_ref, patch_ref, wave_ref,
):
    window = probe_ref.shape[1]
    tile = obj_ref.shape[1]
    for part in range(2):
        for block in range(2):
            cols = slice(block * window, (block + 1) * window)
            ext_ref[part, block, 0:tile, :] = obj_ref[part, :, cols]
            ext_ref[part, block, tile:, :] = low_ref[part, :, cols].astype(F32)
        ext_ref[part, 2, 0:tile, :] = right_ref[part].astype(F32)
        ext_ref[part, 2, tile:, :] = corner_ref[part].astype(F32)
    dep_ref[...] = jnp.zeros(dep_ref.shape, F32)
    power_ref[...] = probe_ref[0] * probe_ref[0] + probe_ref[1] * probe_ref[1]
    sweep_slots(
        live_ref, corners_ref, ext_ref, probe_ref, amp_ref, tab_ref,
        dep_ref, None, power_ref, patch_ref, wave_ref, True,
    )
    for part in range(3):
        to_right_ref[part] = dep_ref[part, 2].astype(TERMS)
        to_left_ref[part] = dep_ref[part, 0].astype(TERMS)


def middle_kernel(dep_ref, from_left_ref, from_right_ref, down_ref, up_ref):
    window = from_left_ref.shape[2]
    tile = from_left_ref.shape[1] - window
    for part in range(3):
        for ref, rows in ((down_ref, slice(tile, tile + window)), (up_ref, slice(0, window))):
            ref[part, 0] = (dep_ref[part, 0, rows, :] + from_left_ref[part, rows, :].astype(F32)).astype(TERMS)
            ref[part, 1] = dep_ref[part, 1, rows, :].astype(TERMS)
            ref[part, 2] = (dep_ref[part, 2, rows, :] + from_right_ref[part, rows, :].astype(F32)).astype(TERMS)


def second_kernel(
    live_ref, corners_ref, ext_ref, dep_in_ref, left_ref, right_ref, above_ref, below_ref,
    probe_ref, amp_ref, tab_ref,
    upd_ref, den_ref, dep_ref, to_right_ref, grad_ref, sum_ref, patch_ref, wave_ref,
):
    window = probe_ref.shape[1]
    total = ext_ref.shape[2]
    tile = total - window
    for block in range(3):
        for first in range(0, total, window):
            rows = slice(first, first + window)
            sums = []
            for part in (2, 0, 1):
                value = dep_in_ref[part, block, rows, :]
                if block == 0:
                    value = value + left_ref[part, rows, :].astype(F32)
                if block == 2:
                    value = value + right_ref[part, rows, :].astype(F32)
                if first == 0:
                    value = value + above_ref[part, block].astype(F32)
                if first == tile:
                    value = value + below_ref[part, block].astype(F32)
                sums.append(value)
            inverse = 1.0 / (sums[0] + 4.0)
            for part in range(2):
                upd_ref[part, block, rows, :] = ext_ref[part, block, rows, :] + sums[part + 1] * inverse
            if first < tile and block < 2:
                den_ref[block, rows, :] = inverse
    dep_ref[...] = jnp.zeros(dep_ref.shape, F32)
    grad_ref[...] = jnp.zeros(grad_ref.shape, F32)
    sweep_slots(
        live_ref, corners_ref, upd_ref, probe_ref, amp_ref, tab_ref,
        dep_ref, grad_ref, None, patch_ref, wave_ref, False,
    )
    for part in range(2):
        to_right_ref[part] = dep_ref[part, 2].astype(TERMS)


def finish_kernel(upd_ref, den_ref, dep_ref, left_ref, above_ref, out_ref):
    window = left_ref.shape[2]
    tile = out_ref.shape[1]
    for part in range(2):
        for block in range(2):
            cols = slice(block * window, (block + 1) * window)
            for first in range(0, tile, window):
                rows = slice(first, first + window)
                value = dep_ref[part, block, rows, :]
                if block == 0:
                    value = value + left_ref[part, rows, :].astype(F32)
                if first == 0:
                    value = value + above_ref[part, block].astype(F32)
                out_ref[part, rows, cols] = (
                    upd_ref[part, block, rows, :] + value * den_ref[block, rows, :]
                )


def probe_kernel(probe_ref, sum_ref, out_ref):
    summed = sum_ref[...]
    power = jnp.sum(summed * summed, axis=(0, 1, 2), keepdims=True)
    scale = 1.0 / jnp.sqrt(power / (out_ref.shape[1] * out_ref.shape[2]) + 1e-06)
    out_ref[...] = probe_ref[...] + summed * scale


VM = pl.BlockSpec(memory_space=pltpu.VMEM)
SM = pl.BlockSpec(memory_space=pltpu.SMEM)


def call(kernel, shapes, in_specs, scratch=(), flops=10**6):
    return pl.pallas_call(
        kernel,
        out_shape=[jax.ShapeDtypeStruct(shape, kind) for shape, kind in shapes],
        in_specs=in_specs,
        out_specs=[VM] * len(shapes),
        scratch_shapes=scratch,
        compiler_params=pltpu.CompilerParams(vmem_limit_bytes=40 * 2**20),
        cost_estimate=pl.CostEstimate(flops=flops, transcendentals=0, bytes_accessed=10**6),
    )


def exchange(parts, axis):
    return lax.all_to_all(parts, axis, 0, 0, tiled=True)


def sweeps(object_field, probe, amplitude, corners, live_count):
    slots = amplitude.shape[2]
    window = probe.shape[1]
    tile = object_field.shape[1]
    wide = tile + window
    across = lax.axis_size("col")
    amp = amplitude.reshape(slots, window, window)
    spots = corners.reshape(2, slots)
    live = live_count.reshape(1, 1)
    tables = dft_tables(window)

    right = shift(object_field[:, :, :window].astype(HALO), "col", -1)
    low = shift(object_field[:, :window, :].astype(HALO), "row", -1)
    diagonal = shift(object_field[:, :window, :window].astype(HALO), ("row", "col"), -(across + 1))
    scratch = [
        pltpu.VMEM((window, window), F32),
        pltpu.VMEM((GROUP, 2, window, window), F32),
        pltpu.VMEM((GROUP, window, 2 * window), BF16),
    ]
    ext, dep, to_right, to_left = call(
        first_kernel,
        [
            ((2, 3, wide, window), F32),
            ((3, 3, wide, window), F32),
            ((3, wide, window), TERMS),
            ((3, wide, window), TERMS),
        ],
        [SM, SM] + [VM] * 7,
        scratch,
        10**9,
    )(live, spots, object_field, right, low, diagonal, probe, amp, tables)

    from_right = shift(to_left, "col", -1)
    from_left = shift(to_right, "col", 1)
    down, up = call(
        middle_kernel, [((3, 3, window, window), TERMS), ((3, 3, window, window), TERMS)], [VM] * 3
    )(dep, from_left, from_right)
    from_below = shift(up, "row", -1)
    from_above = shift(down, "row", 1)

    updated, inverse, dep, to_right, gradient = call(
        second_kernel,
        [
            ((2, 3, wide, window), F32),
            ((2, tile, window), F32),
            ((2, 3, wide, window), F32),
            ((2, wide, window), TERMS),
            ((2, window, window), F32),
        ],
        [SM, SM] + [VM] * 9,
        scratch,
        10**9,
    )(live, spots, ext, dep, from_left, from_right, from_above, from_below, probe, amp, tables)

    rows, cols = lax.axis_size("row"), lax.axis_size("col")
    parts = exchange(gradient.astype(GRAD).reshape(rows, -1, window), "row")
    part = jnp.sum(parts.astype(F32), 0).astype(GRAD)
    to_right, dep, _ = lax.optimization_barrier((to_right, dep, part))
    parts = exchange(jnp.broadcast_to(part[None], (cols,) + part.shape), "col")
    from_left = shift(to_right, "col", 1)
    spill = dep[:, :2, tile:, :]
    spill = jnp.concatenate(
        [(spill[:, :1] + from_left[:, None, tile:].astype(F32)), spill[:, 1:]], 1
    ).astype(TERMS)
    from_above = shift(spill, "row", 1)
    refined = call(
        finish_kernel, [((2, tile, tile), F32)], [VM] * 5
    )(updated, inverse, dep, from_left, from_above)[0]
    parts, refined = lax.optimization_barrier((parts, refined))
    part = jnp.sum(parts.astype(F32), 0)
    parts = exchange(jnp.broadcast_to(part[None], (rows,) + part.shape), "row")
    new_probe = call(probe_kernel, [(probe.shape, F32)], [VM] * 2)(
        probe, parts.reshape(gradient.shape)
    )[0]
    return (refined, new_probe)


def solution(mesh):
    in_specs = (
        P(None, "row", "col"),
        P(),
        P("row", "col", None, None, None),
        P(None, "row", "col", None),
        P("row", "col"),
    )
    out_specs = (P(None, "row", "col"), P())
    return jax.shard_map(sweeps, mesh=mesh, in_specs=in_specs, out_specs=out_specs, check_vma=False)
```
